32 devices in a mesh: groups: 2 (over y), img: 4 (over z), tpl: 2 (over x), sub: 2 (over core).
Axes of the slice: x: 2, y: 2, z: 4, core: 2. Of those that a mesh axis runs over, the one named last changes fastest.
Arguments:
- images: bfloat16 [2048, 4096], P(('groups', 'img', 'tpl', 'sub')), parts along dimension 0, may hold values from -48 to 48
- templates: bfloat16 [4096, 4096], P(('groups', 'tpl', 'sub')), parts along dimension 0, may hold values from -1 to 1, as said below
- group_ids: int32 [2048], P(('groups', 'img')), parts along dimension 0, may hold values from 0 to 31
- group_ctf: float32 [64], P('groups'), parts along dimension 0, may hold values from 1 to 2
- group_prec: float32 [64], P('groups'), parts along dimension 0, may hold values from 1 to 3
- log_prior: float32 [256], P('groups'), parts along dimension 0, may hold values from -4.5 to 4.5
- class_mask: int32 [256], P('groups'), parts along dimension 0, may hold values from 0 to 1
Outputs:
- class_sums: float32 [4096, 4096], P(('groups', 'tpl', 'sub'), 'img'), parts along dimension 0
- evidence: float32 [2048], P(('groups', 'img', 'tpl', 'sub')), parts along dimension 0
The draws below stay inside these ranges and needn't reach their ends.
There are 2 independent parts, one for each index of `groups`. The reference program is written for one: setup_inputs(seed, part) draws one part's arguments, and reference() takes and returns one part's arrays. A program takes and returns all parts, laid end to end along the dimension named above; each array names one. Nothing has to cross between parts.
Inputs may be any that keep to these rules, and one draw needn't show every extreme that they name: `templates`: each row has unit length before rounding.
All inputs are finite; a program needn't handle non-finite values.
Results may differ from the reference program's by a relative error of at most 0.0028.
Values may be sent and summed in bfloat16 or wider, within the bound.
A program may use at most 64 MiB of HBM per device.

```python
import math
import jax
import jax.numpy as jnp
from jax import lax

PIX = 4096
CLASSES = 128
ROTS = 16
CTF_GROUPS = 32
IMG_DEV = 64
IMAGES = 1024
TEMPLATES = 2048
N_TPL = 2
N_SUB = 2


def tables_for(key):
    folded = jax.random.fold_in(key, 7)
    subkeys = jax.random.split(folded, 6)
    group_ids = jax.random.randint(subkeys[0], (IMAGES,), 0, CTF_GROUPS, dtype=jnp.int32)
    group_ctf = jnp.exp(jax.random.uniform(subkeys[1], (CTF_GROUPS,), jnp.float32, 0.0, math.log(2.0)))
    group_prec = jnp.exp(jax.random.uniform(subkeys[2], (CTF_GROUPS,), jnp.float32, 0.0, math.log(3.0)))
    log_prior = jnp.clip(0.7 * jax.random.normal(subkeys[3], (CLASSES,), jnp.float32), -4.5, 4.5)
    forced_class = jax.random.randint(subkeys[4], (), 0, CLASSES, dtype=jnp.int32)
    class_mask = (jax.random.randint(subkeys[5], (CLASSES,), 0, 4, dtype=jnp.int32) > 0).astype(jnp.int32)
    class_mask = jnp.where(jnp.arange(CLASSES, dtype=jnp.int32) == forced_class, 1, class_mask).astype(jnp.int32)
    return (group_ids, group_ctf, group_prec, log_prior, class_mask)


def templates_for(key):
    folded = jax.random.fold_in(key, 13)
    subkeys = jax.random.split(folded, 1)
    raw_field = jax.random.normal(subkeys[0], (TEMPLATES, PIX), jnp.float32)
    return raw_field / jnp.sqrt(jnp.sum(raw_field * raw_field, axis=1, keepdims=True))


def draw_templates(key, part):
    return templates_for(key).astype(jnp.bfloat16)


def draw_group_ids(key, part):
    return tables_for(key)[0]


def draw_group_ctf(key, part):
    return tables_for(key)[1]


def draw_group_prec(key, part):
    return tables_for(key)[2]


def draw_log_prior(key, part):
    return tables_for(key)[3]


def draw_class_mask(key, part):
    return tables_for(key)[4]


def draw_images(key, part):
    folded = jax.random.fold_in(key, 29)
    subkeys = jax.random.split(folded, 2)
    pixel_field = jax.random.normal(subkeys[1], (IMAGES, PIX), jnp.float32)
    return jnp.clip(pixel_field, -48.0, 48.0).astype(jnp.bfloat16)


def setup_inputs(seed: int = 0, part: int = 0) -> dict:
    seeds = jax.random.split(jax.random.key(seed), 8)
    part_keys = jax.random.split(jax.random.fold_in(seeds[7], part), 8)
    return {
        "images": draw_images(jax.random.fold_in(jax.random.fold_in(seeds[7], part), 71), part),
        "templates": draw_templates(jax.random.fold_in(jax.random.fold_in(seeds[7], part), 71), part),
        "group_ids": draw_group_ids(jax.random.fold_in(jax.random.fold_in(seeds[7], part), 71), part),
        "group_ctf": draw_group_ctf(jax.random.fold_in(jax.random.fold_in(seeds[7], part), 71), part),
        "group_prec": draw_group_prec(jax.random.fold_in(jax.random.fold_in(seeds[7], part), 71), part),
        "log_prior": draw_log_prior(jax.random.fold_in(jax.random.fold_in(seeds[7], part), 71), part),
        "class_mask": draw_class_mask(jax.random.fold_in(jax.random.fold_in(seeds[7], part), 71), part),
    }


masked_score = -1.0e30


def scored(raw_dots, tmpl_norm, scale_ctf, scale_prec, prior_rows, active):
    factor = (scale_prec * scale_ctf)[:, None]
    penalty = (0.5 * scale_prec * scale_ctf * scale_ctf)[:, None] * tmpl_norm[None, :]
    values = factor * raw_dots - penalty + prior_rows[None, :]
    return jnp.where(active[None, :], values, masked_score)


def reference(images, templates, group_ids, group_ctf, group_prec, log_prior, class_mask):
    tmpl_norm = jnp.sum(jnp.square(templates.astype(jnp.float32)), axis=1)
    prior_rows = jnp.repeat(log_prior, ROTS)
    active = jnp.repeat(class_mask, ROTS) > 0
    scale_ctf = group_ctf[group_ids]
    scale_prec = group_prec[group_ids]
    block_rows = IMG_DEV * N_TPL * N_SUB
    block_count = IMAGES // block_rows
    block_inputs = (images.reshape(block_count, block_rows, PIX), scale_ctf.reshape(block_count, block_rows), scale_prec.reshape(block_count, block_rows))

    def block_step(running, inputs):
        pixels_in, ctf_in, prec_in = inputs
        raw_dots = lax.dot_general(pixels_in, templates, (((1,), (1,)), ((), ())), preferred_element_type=jnp.float32)
        values = scored(raw_dots, tmpl_norm, ctf_in, prec_in, prior_rows, active)
        score_peak = jnp.max(values, axis=1)
        expo_terms = jnp.where(active[None, :], jnp.exp(values - score_peak[:, None]), 0.0)
        score_total = jnp.sum(expo_terms, axis=1)
        posterior = expo_terms / score_total[:, None]
        weight = (posterior * (prec_in * ctf_in)[:, None]).astype(jnp.bfloat16)
        running = running + lax.dot_general(weight, pixels_in, (((0,), (0,)), ((), ())), preferred_element_type=jnp.float32)
        return running, score_peak + jnp.log(score_total)

    class_sums, evidence = lax.scan(block_step, jnp.zeros((TEMPLATES, PIX), jnp.float32), block_inputs)
    return class_sums, evidence.reshape(IMAGES)
```

```python
import functools
import jax
import jax.numpy as jnp
from jax import lax
from jax.experimental import pallas as pl
from jax.experimental.pallas import tpu as pltpu
from jax.sharding import PartitionSpec as P

ROTS = 16
MASKED = -1e30
PIECES = 2
PARTS = 2
MESH = pl.DeviceIdType.MESH


def exchange_kernel(
    sizes, ids_in, ctf_in, prec_in, prior_in, mask_in, images, templates,
    sums_ref, evid_ref,
    ids_ref, ctf_ref, prec_ref, prior_ref, mask_ref, grid_buf, tmpl, tnorm, base, act, all_w, all_p, own_stat, stat, fac,
    in_sem, tmpl_sem, own_sem, c_send, c_recv, a_send, a_recv, f_send, p_send, p_recv, g_send,
    w_send, w_far, w_recv, s_send, s_recv, v_send, v_recv,
):
    Z, X, C, H, G = sizes
    S = X * C
    g, z, x, c = [lax.axis_index(n) for n in ("groups", "img", "tpl", "sub")]
    refs, nb = tnorm.shape
    classes = refs // ROTS
    rows, pix = grid_buf.shape[2:]
    pb = pix // Z
    hr = rows // H
    gr = refs // G
    s = x * C + c

    def chip(d):
        return lax.rem(x + d, X)

    def core(d):
        return lax.rem(c + d, C)

    def zoff(d):
        return lax.rem(z + d, Z)

    def dev(zz, xx, cc):
        return (g, zz, xx, cc)

    def scope(name):
        return jax.named_scope(name)

    peers = [(dx, dc) for dx in range(X) for dc in range(C) if dx or dc]
    inner = (z > 0) & (z < Z - 1)

    barrier = pltpu.get_barrier_semaphore()
    for dx, dc in peers:
        pl.semaphore_signal(barrier, inc=1, device_id=dev(z, chip(dx), core(dc)), device_id_type=MESH)
    for d in range(1, Z):
        pl.semaphore_signal(barrier, inc=1, device_id=dev(zoff(d), x, c), device_id_type=MESH)

    started = []

    def local(src, dst, sem):
        cp = pltpu.make_async_copy(src, dst, sem)
        cp.start()
        return cp

    def copy(src, dst, send, recv, to):
        return pltpu.make_async_remote_copy(
            src_ref=src, dst_ref=dst, send_sem=send, recv_sem=recv, device_id=to, device_id_type=MESH
        )

    def remote(*args):
        cp = copy(*args)
        cp.start()
        started.append(cp)

    def arrive(dst, sem):
        pltpu.make_async_copy(dst, dst, sem).wait()

    small = [
        local(src, dst, in_sem.at[i])
        for i, (src, dst) in enumerate((
            (ids_in, ids_ref), (ctf_in, ctf_ref), (prec_in, prec_ref), (prior_in, prior_ref), (mask_in, mask_ref),
        ))
    ]
    tmpl_copy = local(templates, tmpl, tmpl_sem)
    own_copy = local(images, grid_buf.at[0, c], own_sem)

    with scope("barrier"):
        pl.semaphore_wait(barrier, S - 1 + Z - 1)

    def piece(i, cc, h):
        return grid_buf.at[i, cc, pl.ds(h * hr, hr), :]

    for dc in range(1, C):
        remote(images, grid_buf.at[0, c], c_send.at[dc - 1], c_recv.at[c], dev(z, x, core(dc)))
    for h in range(H):
        for dx in range(1, X):
            remote(
                images.at[pl.ds(h * hr, hr), :], piece(X - dx, c, h), a_send.at[dx - 1, h], a_recv.at[X - dx, c, h],
                dev(z, chip(dx), c),
            )

    def p_block(zz, i, cc):
        return all_p.at[zz, i, cc]

    def p_copy(d):
        zz = zoff(d)
        cols = pl.ds(pl.multiple_of(zz * pb, pb), pb)
        return copy(images.at[:, cols], p_block(z, 0, c), p_send.at[d - 1], p_recv.at[z, 0, c], dev(zz, x, c))

    def outer(d):
        zz = zoff(d)
        return (zz == 0) | (zz == Z - 1)

    for d in range(1, Z):
        @pl.when(outer(d))
        def _():
            p_copy(d).start()

    with scope("small"):
        for cp in small:
            cp.wait()
    first = s * classes
    for i in range(classes):
        rws = pl.ds(i * ROTS, ROTS)
        base[rws, :] = jnp.full((ROTS, nb), prior_ref[first + i], jnp.float32)
        act[rws, :] = jnp.full((ROTS, nb), mask_ref[first + i], jnp.int32).astype(jnp.float32)

    factors, penalties = [], []
    for i in range(X):
        ids = ids_ref[chip(i)]
        ctf = jnp.zeros(ids.shape, jnp.float32)
        prec = ctf
        for q in range(ctf_ref.shape[0]):
            hit = ids == q
            ctf = jnp.where(hit, ctf_ref[q], ctf)
            prec = jnp.where(hit, prec_ref[q], prec)
        factors.append(prec * ctf)
        penalties.append(0.5 * prec * ctf * ctf)

    with scope("tmplw"):
        tmpl_copy.wait()

    with scope("tnorm"):
        @pl.loop(0, refs // 16)
        def _(i):
            rws = pl.ds(pl.multiple_of(i * 16, 16), 16)
            t = tmpl[rws, :].astype(jnp.float32)
            tnorm[rws, :] = jnp.broadcast_to(jnp.sum(t * t, axis=1, keepdims=True), (16, nb))

    def w_part(i, zz, q):
        return all_w.at[i, zz, pl.ds(q * gr, gr), :]

    def w_go(i, zz, q, right):
        step = 1 if right else -1
        return copy(
            w_part(i, zz, q), w_part(i, zz, q), w_send.at[0 if right else 1, i, zz, q], w_recv.at[i, zz, q],
            dev(lax.rem(z + step + Z, Z), x, c),
        )

    def w_two(i, q):
        zz = lax.rem(jnp.where(z == 0, z + 2, z - 2) + Z, Z)
        return copy(w_part(i, z, q), w_part(i, z, q), w_far.at[i, q], w_recv.at[i, z, q], dev(zz, x, c))

    has_two = ((z == 0) | (z == Z - 1)) if Z > 2 else None

    def forwards(src, right):
        if right:
            return (z < Z - 1) & ((src > 0) | (z != 1))
        return (z > 0) & ((src < Z - 1) | (z != Z - 2))

    def sides(d, fn):
        @pl.when(z - d >= 0)
        def _():
            fn(z - d, True)

        @pl.when(z + d < Z)
        def _():
            fn(z + d, False)

    def w_forward(i):
        def fn(src, right):
            @pl.when(forwards(src, right))
            def _():
                for q in range(G):
                    with scope(f"wf{i}"):
                        arrive(w_part(i, src, q), w_recv.at[i, src, q])
                    w_go(i, src, q, right).start()
        return fn

    def w_wait(i):
        def fn(src, right):
            @pl.when(jnp.logical_not(forwards(src, right)))
            def _():
                for q in range(G):
                    with scope(f"ww{i}"):
                        arrive(w_part(i, src, q), w_recv.at[i, src, q])
        return fn

    def scores(i):
        pixels = grid_buf[i].reshape(nb, pix)
        raw = lax.dot_general(tmpl[...], pixels, (((1,), (1,)), ((), ())), preferred_element_type=jnp.float32)
        live = act[...] > 0.0
        values = jnp.where(live, factors[i] * raw - penalties[i] * tnorm[...] + base[...], MASKED)
        peak = jnp.max(values, axis=0, keepdims=True)
        terms = jnp.where(live, jnp.exp(values - peak), 0.0)
        all_w[i, z] = terms.astype(jnp.bfloat16)
        total = jnp.sum(terms, axis=0, keepdims=True)
        row = lax.broadcasted_iota(jnp.int32, (8, nb), 0)
        own_stat[chip(i)] = jnp.where(row == 0, peak, total)
        for q in range(G):
            if Z > 2:
                @pl.when(has_two)
                def _():
                    w_two(i, q).start()

            @pl.when(z < Z - 1)
            def _():
                w_go(i, z, q, True).start()

            @pl.when(z > 0)
            def _():
                w_go(i, z, q, False).start()

    def p_forward(zz):
        out = []
        for dx in range(1, X):
            out.append(copy(p_block(zz, 0, c), p_block(zz, X - dx, c), g_send.at[zz, dx - 1, 0], p_recv.at[zz, X - dx, c], dev(z, chip(dx), c)))
        for dc in range(1, C):
            out.append(copy(p_block(zz, 0, c), p_block(zz, 0, c), g_send.at[zz, X - 1, dc - 1], p_recv.at[zz, 0, c], dev(z, x, core(dc))))
        return out

    def p_second(zz):
        out = []
        for dx in range(1, X):
            for dc in range(1, C):
                out.append(copy(p_block(zz, dx, c), p_block(zz, dx, c), g_send.at[zz, dx - 1, dc], p_recv.at[zz, dx, c], dev(z, x, core(dc))))
        return out

    def p_start(zz, right):
        with scope("pst"):
            arrive(p_block(zz, 0, c), p_recv.at[zz, 0, c])
        for cp in p_forward(zz):
            cp.start()

    def gather(dx, h):
        with scope(f"gath{h}"):
            arrive(piece(dx, c, h), a_recv.at[dx, c, h])
        for dc in range(1, C):
            remote(piece(dx, c, h), piece(dx, c, h), f_send.at[dx - 1, h, dc - 1], a_recv.at[dx, c, h], dev(z, x, core(dc)))

    own_copy.wait()
    with scope("own"):
        for dc in range(1, C):
            arrive(grid_buf.at[0, core(dc)], c_recv.at[core(dc)])
    with scope("sc0"):
        scores(0)
    for d in range(1, Z):
        @pl.when(jnp.logical_not(outer(d)))
        def _():
            p_copy(d).start()

    early = min(2, Z - 1)
    for dx in range(1, X):
        for h in range(H):
            gather(dx, h)
            if dx == 1 and h == 0:
                sides(1, w_forward(0))

                @pl.when(jnp.logical_not(inner))
                def _():
                    for d in range(1, early + 1):
                        sides(d, p_start)
            elif h == H - 1:
                for d in range(2 if dx == 1 else 1, early + 1):
                    sides(d, w_forward(dx - 1))
        with scope(f"arrA{dx}"):
            for h in range(H):
                for dc in range(1, C):
                    arrive(piece(dx, core(dc), h), a_recv.at[dx, core(dc), h])
        with scope(f"sc{dx}"):
            scores(dx)

    for i, (dx, dc) in enumerate(peers):
        remote(own_stat, stat.at[s], s_send.at[i], s_recv.at[s], dev(z, chip(dx), core(dc)))

    @pl.when(inner)
    def _():
        for d in range(1, early + 1):
            sides(d, p_start)

    @pl.loop(early + 1, Z)
    def _(d):
        sides(d, p_start)

    with scope("stat"):
        for dx, dc in peers:
            slot = chip(dx) * C + core(dc)
            arrive(stat.at[slot], s_recv.at[slot])
    for i in range(X):
        xs = chip(i)
        own = own_stat[xs]
        parts = [(own[0:1], own[1:2])]
        for dx, dc in peers:
            got = stat[chip(dx) * C + core(dc), xs]
            parts.append((got[0:1], got[1:2]))
        peak = functools.reduce(jnp.maximum, [p for p, _ in parts])
        total = functools.reduce(jnp.add, [t * jnp.exp(p - peak) for p, t in parts])
        fac[z, i] = jnp.broadcast_to(factors[i] * jnp.exp(own[0:1] - peak) / total, (8, nb))
        if i == 0:
            evid = peak + jnp.log(total)
            mine = evid[:, 0:rows]
            for q in range(1, C):
                mine = jnp.where(c == q, evid[:, q * rows : (q + 1) * rows], mine)
            evid_ref[...] = mine
    for d in range(1, Z):
        remote(fac.at[z], fac.at[z], v_send.at[d - 1], v_recv.at[z], dev(zoff(d), x, c))

    def weights(zz):
        return jnp.concatenate(
            [(all_w[i, zz].astype(jnp.float32) * fac[zz, i, 0:1]).astype(jnp.bfloat16) for i in range(X)], axis=1
        )

    own_p = grid_buf[:, :, :, pl.ds(pl.multiple_of(z * pb, pb), pb)].reshape(X * nb, pb)
    with scope("prod0"):
        sums_ref[...] = jnp.dot(weights(z), own_p, preferred_element_type=jnp.float32)

    def second_step(src, right):
        for dx in range(1, X):
            with scope("psec"):
                arrive(p_block(src, dx, c), p_recv.at[src, dx, c])
        for cp in p_second(src):
            cp.start()

    def add_step(src, right):
        for i in range(X):
            w_wait(i)(src, right)
        with scope("vw"):
            arrive(fac.at[src], v_recv.at[src])
        with scope("addw"):
            for dx in range(X):
                for dc in range(1, C):
                    arrive(p_block(src, dx, core(dc)), p_recv.at[src, dx, core(dc)])
        with scope("addp"):
            sums_ref[...] += jnp.dot(weights(src), all_p[src].reshape(X * nb, pb), preferred_element_type=jnp.float32)

    @pl.loop(1, Z + 1)
    def _(d):
        @pl.when(d < Z)
        def _():
            for i in range(X - 1):
                @pl.when(d > early)
                def _():
                    sides(d, w_forward(i))
            sides(d, w_forward(X - 1))
            sides(d, second_step)

        @pl.when(d > 1)
        def _():
            sides(d - 1, add_step)

    with scope("drain"):
        for cp in started:
            cp.wait_send()
        for d in range(1, Z):
            p_copy(d).wait_send()

        def end_step(src, right):
            for cp in p_forward(src) + p_second(src):
                cp.wait_send()
            for i in range(X):
                @pl.when(forwards(src, right))
                def _():
                    for q in range(G):
                        w_go(i, src, q, right).wait_send()

        @pl.loop(1, Z)
        def _(d):
            sides(d, end_step)

        for i in range(X):
            for q in range(G):
                if Z > 2:
                    @pl.when(has_two)
                    def _():
                        w_two(i, q).wait_send()

                @pl.when(z < Z - 1)
                def _():
                    w_go(i, z, q, True).wait_send()

                @pl.when(z > 0)
                def _():
                    w_go(i, z, q, False).wait_send()


def exchange(mesh, images, templates, group_ids, group_ctf, group_prec, log_prior, class_mask):
    Z, X, C = mesh.shape["img"], mesh.shape["tpl"], mesh.shape["sub"]
    S = X * C
    rows, pix = images.shape
    refs = templates.shape[0]
    nb = C * rows
    pb = pix // Z
    H, G = PIECES, PARTS
    vmem = pl.BlockSpec(memory_space=pltpu.VMEM)
    anyw = pl.BlockSpec(memory_space=pl.ANY)
    dma = pltpu.SemaphoreType.DMA
    f32, bf16 = jnp.float32, jnp.bfloat16
    x1, c1, z1 = max(X - 1, 1), max(C - 1, 1), max(Z - 1, 1)
    class_sums, evid = pl.pallas_call(
        functools.partial(exchange_kernel, (Z, X, C, H, G)),
        out_shape=(
            pltpu.VMEM((refs, pb), f32),
            pltpu.VMEM((1, rows), f32),
        ),
        in_specs=[anyw] * 7,
        out_specs=(vmem, vmem),
        scratch_shapes=[
            pltpu.VMEM((X, 1, nb), jnp.int32),
            pltpu.SMEM(group_ctf.shape, f32),
            pltpu.SMEM(group_prec.shape, f32),
            pltpu.SMEM(log_prior.shape, f32),
            pltpu.SMEM(class_mask.shape, jnp.int32),
            pltpu.VMEM((X, C, rows, pix), bf16),
            pltpu.VMEM((refs, pix), bf16),
            pltpu.VMEM((refs, nb), f32),
            pltpu.VMEM((refs, nb), f32),
            pltpu.VMEM((refs, nb), f32),
            pltpu.VMEM((X, Z, refs, nb), bf16),
            pltpu.VMEM((Z, X, C, rows, pb), bf16),
            pltpu.VMEM((X, 8, nb), f32),
            pltpu.VMEM((S, X, 8, nb), f32),
            pltpu.VMEM((Z, X, 8, nb), f32),
            dma((5,)), dma(()), dma(()), dma((c1,)), dma((C,)), dma((x1, H)), dma((X, C, H)), dma((x1, H, c1)),
            dma((z1,)), dma((Z, X, C)), dma((Z, X, C)),
            dma((2, X, Z, G)), dma((X, G)), dma((X, Z, G)), dma((max(S - 1, 1),)), dma((S,)), dma((z1,)), dma((Z,)),
        ],
        compiler_params=pltpu.CompilerParams(
            collective_id=0, has_side_effects=True, vmem_limit_bytes=56 * 1024 * 1024
        ),
    )(group_ids.reshape(X, 1, nb), group_ctf, group_prec, log_prior, class_mask, images, templates)
    return class_sums, evid.reshape(rows)


def solution(mesh):
    placed = (
        P(("groups", "img", "tpl", "sub"), None),
        P(("groups", "tpl", "sub"), None),
        P(("groups", "img")),
        P("groups"),
        P("groups"),
        P("groups"),
        P("groups"),
    )
    return jax.shard_map(
        functools.partial(exchange, mesh),
        mesh=mesh,
        in_specs=placed,
        out_specs=(P(("groups", "tpl", "sub"), "img"), P(("groups", "img", "tpl", "sub"))),
        check_vma=False,
    )
```

```python
import functools
import jax
import jax.numpy as jnp
from jax import lax
from jax.experimental import pallas as pl
from jax.experimental.pallas import tpu as pltpu
from jax.sharding import PartitionSpec as P

ROTS = 16
MASKED = -1e30
PIECES = 2
PARTS = 4
NORM = 64
MESH = pl.DeviceIdType.MESH


def exchange_kernel(
    sizes, ids_in, ctf_in, prec_in, prior_in, mask_in, images, templates,
    sums_ref, evid_ref,
    ids_ref, ctf_ref, prec_ref, prior_ref, mask_ref, grid_buf, tmpl, tnorm, base, act, all_w, all_p, own_stat, stat, fac,
    in_sem, tmpl_sem, own_sem, sent, c_recv, a_recv, p_recv, w_recv, s_recv, v_recv, up,
):
    Z, X, C, H, G = sizes
    S = X * C
    g, z, x, c = [lax.axis_index(n) for n in ("groups", "img", "tpl", "sub")]
    refs, nb = tnorm.shape
    classes = refs // ROTS
    rows, pix = grid_buf.shape[2:]
    pb = pix // Z
    hr = rows // H
    gr = refs // G
    s = x * C + c

    def chip(d):
        return lax.rem(x + d, X)

    def core(d):
        return lax.rem(c + d, C)

    def zoff(d):
        return lax.rem(z + d, Z)

    def dev(zz, xx, cc):
        return (g, zz, xx, cc)

    def scope(name):
        return jax.named_scope(name)

    peers = [(dx, dc) for dx in range(X) for dc in range(C) if dx or dc]
    inner = (z > 0) & (z < Z - 1)
    early = min(2, Z - 1)

    barrier = pltpu.get_barrier_semaphore()
    for dx, dc in peers:
        pl.semaphore_signal(barrier, inc=1, device_id=dev(z, chip(dx), core(dc)), device_id_type=MESH)

    @pl.loop(z + 1, Z)
    def _(zz):
        pl.semaphore_signal(barrier, inc=1, device_id=dev(zz, x, c), device_id_type=MESH)

    started = []

    def local(src, dst, sem):
        cp = pltpu.make_async_copy(src, dst, sem)
        cp.start()
        return cp

    def copy(src, dst, send, recv, to):
        return pltpu.make_async_remote_copy(
            src_ref=src, dst_ref=dst, send_sem=send, recv_sem=recv, device_id=to, device_id_type=MESH
        )

    def remote(*args):
        cp = copy(*args)
        cp.start()
        started.append(cp)

    def arrive(dst, sem):
        pltpu.make_async_copy(dst, dst, sem).wait()

    small = [
        local(src, dst, in_sem.at[i])
        for i, (src, dst) in enumerate((
            (ids_in, ids_ref), (ctf_in, ctf_ref), (prec_in, prec_ref), (prior_in, prior_ref), (mask_in, mask_ref),
        ))
    ]
    tmpl_copy = local(templates, tmpl, tmpl_sem)
    own_copy = local(images, grid_buf.at[0, c], own_sem)

    with scope("barrier"):
        pl.semaphore_wait(barrier, S - 1 + z)

    @pl.loop(0, z)
    def _(zz):
        pl.semaphore_signal(up.at[z], inc=1, device_id=dev(zz, x, c), device_id_type=MESH)

    def piece(i, cc, h):
        return grid_buf.at[i, cc, pl.ds(h * hr, hr), :]

    for dc in range(1, C):
        remote(images, grid_buf.at[0, c], sent, c_recv.at[c], dev(z, x, core(dc)))
    for h in range(H):
        for dx in range(1, X):
            remote(
                images.at[pl.ds(h * hr, hr), :], piece(X - dx, c, h), sent, a_recv.at[X - dx, c, h],
                dev(z, chip(dx), c),
            )

    def p_block(zz, i, cc):
        return all_p.at[zz, i, cc]

    def p_copy(d):
        zz = zoff(d)
        cols = pl.ds(pl.multiple_of(zz * pb, pb), pb)
        return copy(images.at[:, cols], p_block(z, 0, c), sent, p_recv.at[z, 0, c], dev(zz, x, c))

    def outer(d):
        zz = zoff(d)
        return (zz == 0) | (zz == Z - 1)

    def crosses(zz):
        return (2 * z < Z) != (2 * zz < Z)

    def p_send_inner(late):
        for d in range(1, Z):
            over = crosses(zoff(d)) & jnp.logical_not(inner)
            first = (z == 0) & (zoff(d) == 1)

            @pl.when(jnp.logical_not(outer(d) | first) & (over if late else jnp.logical_not(over)))
            def _():
                p_copy(d).start()

    for d in range(1, Z):
        @pl.when(zoff(d) == 0)
        def _():
            p_copy(d).start()

    with scope("small"):
        for cp in small:
            cp.wait()
    first = s * classes
    for i in range(classes):
        rws = pl.ds(i * ROTS, ROTS)
        base[rws, :] = jnp.full((ROTS, nb), prior_ref[first + i], jnp.float32)
        act[rws, :] = jnp.full((ROTS, nb), mask_ref[first + i], jnp.int32).astype(jnp.float32)

    factors, penalties = [], []
    for i in range(X):
        ids = ids_ref[chip(i)]
        ctf = jnp.zeros(ids.shape, jnp.float32)
        prec = ctf
        for q in range(ctf_ref.shape[0]):
            hit = ids == q
            ctf = jnp.where(hit, ctf_ref[q], ctf)
            prec = jnp.where(hit, prec_ref[q], prec)
        factors.append(prec * ctf)
        penalties.append(0.5 * prec * ctf * ctf)

    with scope("tmplw"):
        tmpl_copy.wait()

    with scope("tnorm"):
        @pl.loop(0, refs // NORM)
        def _(i):
            rws = pl.ds(pl.multiple_of(i * NORM, NORM), NORM)
            t = tmpl[rws, :].astype(jnp.float32)
            tnorm[rws, :] = jnp.broadcast_to(jnp.sum(t * t, axis=1, keepdims=True), (NORM, nb))

    def p_far(first):
        @pl.loop(first, Z)
        def _(zz):
            pl.semaphore_wait(up.at[zz], 1)

        for d in range(1, Z):
            @pl.when(zoff(d) == Z - 1)
            def _():
                p_copy(d).start()

    with scope("up"):
        if Z > 2:
            @pl.when(z == 0)
            def _():
                pl.semaphore_wait(up.at[1], 1)
                p_copy(1).start()

            @pl.when(z > 0)
            def _():
                p_far(z + 1)

    def w_part(i, zz, q):
        return all_w.at[i, zz, pl.ds(q * gr, gr), :]

    def w_go(i, zz, q, right):
        step = 1 if right else -1
        return copy(
            w_part(i, zz, q), w_part(i, zz, q), sent, w_recv.at[i, zz, q],
            dev(lax.rem(z + step + Z, Z), x, c),
        )

    def w_two(i, q):
        zz = lax.rem(jnp.where(z == 0, z + 2, z - 2) + Z, Z)
        return copy(w_part(i, z, q), w_part(i, z, q), sent, w_recv.at[i, z, q], dev(zz, x, c))

    has_two = ((z == 0) | (z == Z - 1)) if Z > 2 else None

    def forwards(src, right):
        if right:
            return (z < Z - 1) & ((src > 0) | (z != 1))
        return (z > 0) & ((src < Z - 1) | (z != Z - 2))

    def sides(d, fn):
        @pl.when(z - d >= 0)
        def _():
            fn(z - d, True)

        @pl.when(z + d < Z)
        def _():
            fn(z + d, False)

    def w_forward(i, q):
        def fn(src, right):
            @pl.when(forwards(src, right))
            def _():
                with scope(f"wf{i}"):
                    arrive(w_part(i, src, q), w_recv.at[i, src, q])
                w_go(i, src, q, right).start()
        return fn

    def w_forwards(i, d, side, parts=range(G)):
        def fn(src, right):
            if side is None or side == right:
                for q in parts:
                    w_forward(i, q)(src, right)
        sides(d, fn)

    def w_wait(i, q):
        def fn(src, right):
            @pl.when(jnp.logical_not(forwards(src, right)))
            def _():
                with scope(f"ww{i}"):
                    arrive(w_part(i, src, q), w_recv.at[i, src, q])
        return fn

    def scores(i):
        pixels = grid_buf[i].reshape(nb, pix)
        raw = lax.dot_general(pixels, tmpl[...], (((1,), (1,)), ((), ())), preferred_element_type=jnp.float32).T
        live = act[...] > 0.0
        values = jnp.where(live, factors[i] * raw - penalties[i] * tnorm[...] + base[...], MASKED)
        peak = jnp.max(values, axis=0, keepdims=True)
        terms = jnp.where(live, jnp.exp(values - peak), 0.0)
        all_w[i, z] = terms.astype(jnp.bfloat16)
        total = jnp.sum(terms, axis=0, keepdims=True)
        row = lax.broadcasted_iota(jnp.int32, (8, nb), 0)
        own_stat[chip(i)] = jnp.where(row == 0, peak, total)

    def w_start(i):
        for q in range(G):
            if Z > 2:
                @pl.when(has_two)
                def _():
                    w_two(i, q).start()

            @pl.when(z < Z - 1)
            def _():
                w_go(i, z, q, True).start()

            @pl.when(z > 0)
            def _():
                w_go(i, z, q, False).start()

    def p_forward(zz):
        out = []
        for dx in range(1, X):
            out.append(copy(p_block(zz, 0, c), p_block(zz, X - dx, c), sent, p_recv.at[zz, X - dx, c], dev(z, chip(dx), c)))
        for dc in range(1, C):
            out.append(copy(p_block(zz, 0, c), p_block(zz, 0, c), sent, p_recv.at[zz, 0, c], dev(z, x, core(dc))))
        return out

    def p_second(zz):
        out = []
        for dx in range(1, X):
            for dc in range(1, C):
                out.append(copy(p_block(zz, dx, c), p_block(zz, dx, c), sent, p_recv.at[zz, dx, c], dev(z, x, core(dc))))
        return out

    def p_start(zz, right):
        with scope("pst"):
            arrive(p_block(zz, 0, c), p_recv.at[zz, 0, c])
        for cp in p_forward(zz):
            cp.start()

    def p_slot(d, n):
        def fn(src, right):
            slot = jnp.where(inner & crosses(src), 2, jnp.where(inner | (d == 1), 0, 1))

            @pl.when(slot == n)
            def _():
                p_start(src, right)
        sides(d, fn)

    def gather(dx, h):
        with scope(f"gath{h}"):
            arrive(piece(dx, c, h), a_recv.at[dx, c, h])
        for dc in range(1, C):
            remote(piece(dx, c, h), piece(dx, c, h), sent, a_recv.at[dx, c, h], dev(z, x, core(dc)))

    own_copy.wait()
    with scope("own"):
        for dc in range(1, C):
            arrive(grid_buf.at[0, core(dc)], c_recv.at[core(dc)])
    with scope("sc0"):
        scores(0)

    @pl.when(z == 0)
    def _():
        p_far(min(2, Z - 1))

    w_start(0)
    p_send_inner(False)

    for dx in range(1, X):
        for h in range(H):
            gather(dx, h)
            if h == H - 2:
                for d in range(early, 1, -1):
                    w_forwards(dx - 1, d, False)
                w_forwards(dx - 1, 1, False, range(G // 2))
            elif h == H - 1:
                w_forwards(dx - 1, 1, False, range(G // 2, G))
        if dx == X - 1:
            p_send_inner(True)
            for d in range(1, early + 1):
                p_slot(d, 0)
        with scope(f"arrA{dx}"):
            for h in range(H):
                for dc in range(1, C):
                    arrive(piece(dx, core(dc), h), a_recv.at[dx, core(dc), h])
        with scope(f"sc{dx}"):
            scores(dx)
        w_start(dx)

    for i, (dx, dc) in enumerate(peers):
        remote(own_stat, stat.at[s], sent, s_recv.at[s], dev(z, chip(dx), core(dc)))

    for d in range(1, early + 1):
        p_slot(d, 1)

    @pl.loop(early + 1, Z)
    def _(d):
        sides(d, p_start)

    with scope("stat"):
        for dx, dc in peers:
            slot = chip(dx) * C + core(dc)
            arrive(stat.at[slot], s_recv.at[slot])
    for i in range(X):
        xs = chip(i)
        own = own_stat[xs]
        parts = [(own[0:1], own[1:2])]
        for dx, dc in peers:
            got = stat[chip(dx) * C + core(dc), xs]
            parts.append((got[0:1], got[1:2]))
        peak = functools.reduce(jnp.maximum, [p for p, _ in parts])
        total = functools.reduce(jnp.add, [t * jnp.exp(p - peak) for p, t in parts])
        fac[z, i] = jnp.broadcast_to(factors[i] * jnp.exp(own[0:1] - peak) / total, (8, nb))
        if i == 0:
            evid = peak + jnp.log(total)
            mine = evid[:, 0:rows]
            for q in range(1, C):
                mine = jnp.where(c == q, evid[:, q * rows : (q + 1) * rows], mine)
            evid_ref[...] = mine
    for d in range(1, Z):
        remote(fac.at[z], fac.at[z], sent, v_recv.at[z], dev(zoff(d), x, c))

    def weights(zz, chunks, rws):
        return jnp.concatenate(
            [(all_w[i, zz, rws, :].astype(jnp.float32) * fac[zz, i, 0:1]).astype(jnp.bfloat16) for i in chunks], axis=1
        )

    def product(zz, chunks, rws):
        block = all_p[zz, chunks[0] : chunks[-1] + 1].reshape(len(chunks) * nb, pb)
        sums_ref[rws, :] += jnp.dot(weights(zz, chunks, rws), block, preferred_element_type=jnp.float32)

    def second_step(src, right):
        for dx in range(1, X):
            with scope("psec"):
                arrive(p_block(src, dx, c), p_recv.at[src, dx, c])
        for cp in p_second(src):
            cp.start()

    def add_step(chunks):
        def fn(src, right):
            for i in chunks:
                for q in range(G):
                    w_wait(i, q)(src, right)
            with scope("vw"):
                arrive(fac.at[src], v_recv.at[src])
            with scope("addw"):
                for dx in range(X):
                    for dc in range(1, C):
                        arrive(p_block(src, dx, core(dc)), p_recv.at[src, dx, core(dc)])
            with scope("addp"):
                product(src, chunks, pl.ds(0, refs))
        return fn

    def last_step(q):
        def fn(src, right):
            w_wait(X - 1, q)(src, right)
            with scope(f"last{q}"):
                product(src, range(X - 1, X), pl.ds(q * gr, gr))
        return fn

    for i in range(X - 1):
        for d in range(early, 0, -1):
            w_forwards(i, d, True)
    for d in range(early, 0, -1):
        p_slot(d, 2)
        if d > 1:
            w_forwards(X - 1, d, None)
    w_forwards(X - 1, 1, None)

    @pl.loop(early + 1, Z)
    def _(d):
        for i in range(X):
            w_forwards(i, d, None)

    own_p = grid_buf[:, :, :, pl.ds(pl.multiple_of(z * pb, pb), pb)].reshape(X * nb, pb)
    with scope("prod0"):
        sums_ref[...] = jnp.dot(weights(z, range(X), pl.ds(0, refs)), own_p, preferred_element_type=jnp.float32)

    for d in range(1, early + 1):
        sides(d, second_step)

    @pl.loop(early + 1, Z)
    def _(d):
        sides(d, second_step)

    sides(1, add_step(range(X)))

    @pl.loop(2, Z)
    def _(d):
        sides(d, add_step(range(max(X - 1, 1))))

    if X > 1:
        @pl.loop(0, Z - 2)
        def _(d):
            for q in range(G):
                sides(Z - 1 - d, last_step(q))

    with scope("drain"):
        for cp in started:
            cp.wait_send()
        for d in range(1, Z):
            p_copy(d).wait_send()

        def end_step(src, right):
            for cp in p_forward(src) + p_second(src):
                cp.wait_send()
            for i in range(X):
                @pl.when(forwards(src, right))
                def _():
                    for q in range(G):
                        w_go(i, src, q, right).wait_send()

        @pl.loop(1, Z)
        def _(d):
            sides(d, end_step)

        for i in range(X):
            for q in range(G):
                if Z > 2:
                    @pl.when(has_two)
                    def _():
                        w_two(i, q).wait_send()

                @pl.when(z < Z - 1)
                def _():
                    w_go(i, z, q, True).wait_send()

                @pl.when(z > 0)
                def _():
                    w_go(i, z, q, False).wait_send()


def exchange(mesh, images, templates, group_ids, group_ctf, group_prec, log_prior, class_mask):
    Z, X, C = mesh.shape["img"], mesh.shape["tpl"], mesh.shape["sub"]
    S = X * C
    rows, pix = images.shape
    refs = templates.shape[0]
    nb = C * rows
    pb = pix // Z
    H, G = PIECES, PARTS
    vmem = pl.BlockSpec(memory_space=pltpu.VMEM)
    anyw = pl.BlockSpec(memory_space=pl.ANY)
    dma = pltpu.SemaphoreType.DMA
    f32, bf16 = jnp.float32, jnp.bfloat16
    class_sums, evid = pl.pallas_call(
        functools.partial(exchange_kernel, (Z, X, C, H, G)),
        out_shape=(
            pltpu.VMEM((refs, pb), f32),
            pltpu.VMEM((1, rows), f32),
        ),
        in_specs=[anyw] * 7,
        out_specs=(vmem, vmem),
        scratch_shapes=[
            pltpu.VMEM((X, 1, nb), jnp.int32),
            pltpu.SMEM(group_ctf.shape, f32),
            pltpu.SMEM(group_prec.shape, f32),
            pltpu.SMEM(log_prior.shape, f32),
            pltpu.SMEM(class_mask.shape, jnp.int32),
            pltpu.VMEM((X, C, rows, pix), bf16),
            pltpu.VMEM((refs, pix), bf16),
            pltpu.VMEM((refs, nb), f32),
            pltpu.VMEM((refs, nb), f32),
            pltpu.VMEM((refs, nb), f32),
            pltpu.VMEM((X, Z, refs, nb), bf16),
            pltpu.VMEM((Z, X, C, rows, pb), bf16),
            pltpu.VMEM((X, 8, nb), f32),
            pltpu.VMEM((S, X, 8, nb), f32),
            pltpu.VMEM((Z, X, 8, nb), f32),
            dma((5,)), dma(()), dma(()), dma(()), dma((C,)), dma((X, C, H)), dma((Z, X, C)), dma((X, Z, G)), dma((S,)), dma((Z,)),
            pltpu.SemaphoreType.REGULAR((Z,)),
        ],
        compiler_params=pltpu.CompilerParams(
            collective_id=0, has_side_effects=True, vmem_limit_bytes=56 * 1024 * 1024
        ),
    )(group_ids.reshape(X, 1, nb), group_ctf, group_prec, log_prior, class_mask, images, templates)
    return class_sums, evid.reshape(rows)


def solution(mesh):
    placed = (
        P(("groups", "img", "tpl", "sub"), None),
        P(("groups", "tpl", "sub"), None),
        P(("groups", "img")),
        P("groups"),
        P("groups"),
        P("groups"),
        P("groups"),
    )
    return jax.shard_map(
        functools.partial(exchange, mesh),
        mesh=mesh,
        in_specs=placed,
        out_specs=(P(("groups", "tpl", "sub"), "img"), P(("groups", "img", "tpl", "sub"))),
        check_vma=False,
    )
```

```python
import functools
import jax
import jax.numpy as jnp
from jax import lax
from jax.experimental import pallas as pl
from jax.experimental.pallas import tpu as pltpu
from jax.sharding import PartitionSpec as P

ROTS = 16
MASKED = -1e30
PIECES = 2
PARTS = 4
NORM = 64
FLUSH = 4
MESH = pl.DeviceIdType.MESH


def exchange_kernel(
    sizes, ids_in, ctf_in, prec_in, prior_in, mask_in, images, templates,
    sums_ref, evid_ref,
    ids_ref, ctf_ref, prec_ref, prior_ref, mask_ref, grid_buf, tmpl, tnorm, base, act, all_w, all_p, own_stat, stat, fac,
    in_sem, tmpl_sem, own_sem, sent, c_recv, a_recv, p_recv, w_recv, s_recv, v_recv, up,
):
    Z, X, C, H, G = sizes
    S = X * C
    g, z, x, c = [lax.axis_index(n) for n in ("groups", "img", "tpl", "sub")]
    refs, nb = tnorm.shape
    classes = refs // ROTS
    rows, pix = grid_buf.shape[2:]
    pb = pix // Z
    hr = rows // H
    gr = refs // G
    s = x * C + c

    def chip(d):
        return lax.rem(x + d, X)

    def core(d):
        return lax.rem(c + d, C)

    def zoff(d):
        return lax.rem(z + d, Z)

    def dev(zz, xx, cc):
        return (g, zz, xx, cc)

    def scope(name):
        return jax.named_scope(name)

    peers = [(dx, dc) for dx in range(X) for dc in range(C) if dx or dc]
    inner = (z > 0) & (z < Z - 1)
    early = min(2, Z - 1)

    barrier = pltpu.get_barrier_semaphore()
    for dx, dc in peers:
        pl.semaphore_signal(barrier, inc=1, device_id=dev(z, chip(dx), core(dc)), device_id_type=MESH)

    @pl.loop(z + 1, Z)
    def _(zz):
        pl.semaphore_signal(barrier, inc=1, device_id=dev(zz, x, c), device_id_type=MESH)

    started = []

    def local(src, dst, sem):
        cp = pltpu.make_async_copy(src, dst, sem)
        cp.start()
        return cp

    def copy(src, dst, send, recv, to):
        return pltpu.make_async_remote_copy(
            src_ref=src, dst_ref=dst, send_sem=send, recv_sem=recv, device_id=to, device_id_type=MESH
        )

    def remote(*args):
        cp = copy(*args)
        cp.start()
        started.append(cp)

    def arrive(dst, sem):
        pltpu.make_async_copy(dst, dst, sem).wait()

    small = [
        local(src, dst, in_sem.at[i])
        for i, (src, dst) in enumerate((
            (ids_in, ids_ref), (ctf_in, ctf_ref), (prec_in, prec_ref), (prior_in, prior_ref), (mask_in, mask_ref),
        ))
    ]
    tmpl_copy = local(templates, tmpl, tmpl_sem)
    own_copy = local(images, grid_buf.at[0, c], own_sem)

    with scope("barrier"):
        pl.semaphore_wait(barrier, S - 1 + z)

    @pl.loop(0, z)
    def _(zz):
        pl.semaphore_signal(up.at[z], inc=1, device_id=dev(zz, x, c), device_id_type=MESH)

    def piece(i, cc, h):
        return grid_buf.at[i, cc, pl.ds(h * hr, hr), :]

    for dc in range(1, C):
        remote(images, grid_buf.at[0, c], sent, c_recv.at[c], dev(z, x, core(dc)))
    for h in range(H):
        for dx in range(1, X):
            remote(
                images.at[pl.ds(h * hr, hr), :], piece(X - dx, c, h), sent, a_recv.at[X - dx, h],
                dev(z, chip(dx), c),
            )

    def p_block(zz, i, cc):
        return all_p.at[zz, i, cc]

    def p_copy(d):
        zz = zoff(d)
        cols = pl.ds(pl.multiple_of(zz * pb, pb), pb)
        return copy(images.at[:, cols], p_block(z, 0, c), sent, p_recv.at[z, 0], dev(zz, x, c))

    def outer(d):
        zz = zoff(d)
        return (zz == 0) | (zz == Z - 1)

    def crosses(zz):
        return (2 * z < Z) != (2 * zz < Z)

    def p_send_inner(n):
        for d in range(1, Z):
            over = crosses(zoff(d)) & jnp.logical_not(inner)
            first = (z == 0) & (zoff(d) == 1)
            slot = jnp.where(over, jnp.where(z == 0, 2, 1), 0)

            @pl.when(jnp.logical_not(outer(d) | first) & (slot == n))
            def _():
                p_copy(d).start()

    for d in range(1, Z):
        @pl.when(zoff(d) == 0)
        def _():
            p_copy(d).start()

    with scope("small"):
        for cp in small:
            cp.wait()
    first = s * classes
    for i in range(classes):
        rws = pl.ds(i * ROTS, ROTS)
        base[rws, :] = jnp.full((ROTS, nb), prior_ref[first + i], jnp.float32)
        act[rws, :] = jnp.full((ROTS, nb), mask_ref[first + i], jnp.int32).astype(jnp.float32)

    factors, penalties = [], []
    for i in range(X):
        ids = ids_ref[chip(i)]
        ctf = jnp.zeros(ids.shape, jnp.float32)
        prec = ctf
        for q in range(ctf_ref.shape[0]):
            hit = ids == q
            ctf = jnp.where(hit, ctf_ref[q], ctf)
            prec = jnp.where(hit, prec_ref[q], prec)
        factors.append(prec * ctf)
        penalties.append(0.5 * prec * ctf * ctf)

    with scope("tmplw"):
        tmpl_copy.wait()

    with scope("tnorm"):
        @pl.loop(0, refs // NORM)
        def _(i):
            rws = pl.ds(pl.multiple_of(i * NORM, NORM), NORM)
            t = tmpl[rws, :].astype(jnp.float32)
            tnorm[rws, :] = jnp.broadcast_to(jnp.sum(t * t, axis=1, keepdims=True), (NORM, nb))

    def p_far(first):
        @pl.loop(first, Z)
        def _(zz):
            pl.semaphore_wait(up.at[zz], 1)

        for d in range(1, Z):
            @pl.when(zoff(d) == Z - 1)
            def _():
                p_copy(d).start()

    with scope("up"):
        if Z > 2:
            @pl.when(z == 0)
            def _():
                pl.semaphore_wait(up.at[1], 1)
                p_copy(1).start()

            @pl.when(z > 0)
            def _():
                p_far(z + 1)

    def w_part(i, zz, q):
        return all_w.at[i, zz, pl.ds(q * gr, gr), :]

    def w_sem(i, src, dst, q):
        return w_recv.at[i, lax.rem(src - dst + Z - 1, Z), q]

    def w_go(i, zz, q, right):
        to = lax.rem(z + (1 if right else -1) + Z, Z)
        return copy(w_part(i, zz, q), w_part(i, zz, q), sent, w_sem(i, zz, to, q), dev(to, x, c))

    def w_two(i, q):
        zz = lax.rem(jnp.where(z == 0, z + 2, z - 2) + Z, Z)
        return copy(w_part(i, z, q), w_part(i, z, q), sent, w_sem(i, z, zz, q), dev(zz, x, c))

    has_two = ((z == 0) | (z == Z - 1)) if Z > 2 else None

    def forwards(src, right):
        if right:
            return (z < Z - 1) & ((src > 0) | (z != 1))
        return (z > 0) & ((src < Z - 1) | (z != Z - 2))

    def sides(d, fn):
        @pl.when(z - d >= 0)
        def _():
            fn(z - d, True)

        @pl.when(z + d < Z)
        def _():
            fn(z + d, False)

    def w_forward(i, q):
        def fn(src, right):
            @pl.when(forwards(src, right))
            def _():
                with scope(f"wf{i}"):
                    arrive(w_part(i, src, q), w_sem(i, src, z, q))
                w_go(i, src, q, right).start()
        return fn

    def w_forwards(i, d, side, parts=range(G)):
        def fn(src, right):
            if side is None or side == right:
                for q in parts:
                    w_forward(i, q)(src, right)
        sides(d, fn)

    def w_wait(i, q):
        def fn(src, right):
            @pl.when(jnp.logical_not(forwards(src, right)))
            def _():
                with scope(f"ww{i}"):
                    arrive(w_part(i, src, q), w_sem(i, src, z, q))
        return fn

    def scores(i):
        pixels = grid_buf[i].reshape(nb, pix)
        raw = lax.dot_general(pixels, tmpl[...], (((1,), (1,)), ((), ())), preferred_element_type=jnp.float32).T
        live = act[...] > 0.0
        values = jnp.where(live, factors[i] * raw - penalties[i] * tnorm[...] + base[...], MASKED)
        peak = jnp.max(values, axis=0, keepdims=True)
        terms = jnp.where(live, jnp.exp(values - peak), 0.0)
        all_w[i, z] = terms.astype(jnp.bfloat16)
        total = jnp.sum(terms, axis=0, keepdims=True)
        row = lax.broadcasted_iota(jnp.int32, (8, nb), 0)
        own_stat[chip(i)] = jnp.where(row == 0, peak, total)

    def w_start(i):
        if i == X - 1:
            p_send_inner(2)

        if Z > 2:
            @pl.when(has_two)
            def _():
                for q in range(G):
                    w_two(i, q).start()

        for q in range(G):
            @pl.when(z < Z - 1)
            def _():
                w_go(i, z, q, True).start()

            @pl.when(z > 0)
            def _():
                w_go(i, z, q, False).start()

    def p_forward(zz):
        out = []
        for dx in range(1, X):
            out.append(copy(p_block(zz, 0, c), p_block(zz, X - dx, c), sent, p_recv.at[zz, X - dx], dev(z, chip(dx), c)))
        for dc in range(1, C):
            out.append(copy(p_block(zz, 0, c), p_block(zz, 0, c), sent, p_recv.at[zz, X + C - 1 - dc], dev(z, x, core(dc))))
        return out

    def p_second(zz):
        out = []
        for dx in range(1, X):
            for dc in range(1, C):
                out.append(copy(p_block(zz, dx, c), p_block(zz, dx, c), sent, p_recv.at[zz, X + C - 1 - dc], dev(z, x, core(dc))))
        return out

    def p_start(zz, right):
        with scope("pst"):
            arrive(p_block(zz, 0, c), p_recv.at[zz, 0])
        for cp in p_forward(zz):
            cp.start()

    def p_slot(d, n):
        def fn(src, right):
            far = 3 if d == 1 else 2
            slot = jnp.where(inner & crosses(src), far, jnp.where(inner | (d == 1), 0, 1))

            @pl.when(slot == n)
            def _():
                p_start(src, right)
        sides(d, fn)

    def gather(dx, h):
        with scope(f"gath{h}"):
            arrive(piece(dx, c, h), a_recv.at[dx, h])
        for dc in range(1, C):
            remote(piece(dx, c, h), piece(dx, c, h), sent, a_recv.at[dx, H + C - 1 - dc], dev(z, x, core(dc)))

    own_copy.wait()
    with scope("own"):
        for dc in range(1, C):
            arrive(grid_buf.at[0, core(dc)], c_recv.at[core(dc)])
    with scope("sc0"):
        scores(0)

    @pl.when(z == 0)
    def _():
        p_far(min(2, Z - 1))

    w_start(0)
    if X == 1:
        p_send_inner(1)
    p_send_inner(0)

    for dx in range(1, X):
        for h in range(H):
            gather(dx, h)
            if h == H - 2:
                for d in range(early, 1, -1):
                    w_forwards(dx - 1, d, False)
                    w_forwards(dx - 1, d, True, range(G - 1))
                w_forwards(dx - 1, 1, False, range(G // 2))
            elif h == H - 1:
                for d in range(early, 1, -1):
                    w_forwards(dx - 1, d, True, range(G - 1, G))
                w_forwards(dx - 1, 1, False, range(G // 2, G))
        if dx == X - 1:
            p_send_inner(1)
            for d in range(1, early + 1):
                p_slot(d, 0)
        with scope(f"arrA{dx}"):
            for dc in range(1, C):
                arrive(grid_buf.at[dx, core(dc)], a_recv.at[dx, H + dc - 1])
        with scope(f"sc{dx}"):
            scores(dx)
        w_start(dx)

    for dx, dc in peers:
        remote(own_stat, stat.at[s], sent, s_recv, dev(z, chip(dx), core(dc)))

    for i in range(X - 1):
        w_forwards(i, 1, True)
    for d in range(1, early + 1):
        p_slot(d, 1)

    @pl.loop(early + 1, Z)
    def _(d):
        sides(d, p_start)

    with scope("stat"):
        arrive(stat.at[pl.ds(0, S - 1)], s_recv)
    for i in range(X):
        xs = chip(i)
        own = own_stat[xs]
        parts = [(own[0:1], own[1:2])]
        for dx, dc in peers:
            got = stat[chip(dx) * C + core(dc), xs]
            parts.append((got[0:1], got[1:2]))
        peak = functools.reduce(jnp.maximum, [p for p, _ in parts])
        total = functools.reduce(jnp.add, [t * jnp.exp(p - peak) for p, t in parts])
        fac[z, i] = jnp.broadcast_to(factors[i] * jnp.exp(own[0:1] - peak) / total, (8, nb))
        if i == 0:
            evid = peak + jnp.log(total)
            mine = evid[:, 0:rows]
            for q in range(1, C):
                mine = jnp.where(c == q, evid[:, q * rows : (q + 1) * rows], mine)
            evid_ref[...] = mine
    for d in range(1, Z):
        remote(fac.at[z], fac.at[z], sent, v_recv.at[z], dev(zoff(d), x, c))

    def weights(zz, chunks, rws):
        return jnp.concatenate(
            [(all_w[i, zz, rws, :].astype(jnp.float32) * fac[zz, i, 0:1]).astype(jnp.bfloat16) for i in chunks], axis=1
        )

    def product(zz, chunks, rws):
        block = all_p[zz, chunks[0] : chunks[-1] + 1].reshape(len(chunks) * nb, pb)
        sums_ref[rws, :] += jnp.dot(weights(zz, chunks, rws), block, preferred_element_type=jnp.float32)

    def second_step(src, right):
        for dx in range(1, X):
            with scope("psec"):
                arrive(p_block(src, dx, c), p_recv.at[src, dx])
        for cp in p_second(src):
            cp.start()

    def add_step(chunks):
        def fn(src, right):
            for i in chunks:
                for q in range(G):
                    w_wait(i, q)(src, right)
            with scope("vw"):
                arrive(fac.at[src], v_recv.at[src])
            with scope("addw"):
                for dc in range(1, C):
                    arrive(all_p.at[src, :, core(dc)], p_recv.at[src, X + dc - 1])
            with scope("addp"):
                product(src, chunks, pl.ds(0, refs))
        return fn

    def last_step(q):
        def fn(src, right):
            w_wait(X - 1, q)(src, right)
            with scope(f"last{q}"):
                product(src, range(X - 1, X), pl.ds(q * gr, gr))
        return fn

    own_p = grid_buf[:, :, :, pl.ds(pl.multiple_of(z * pb, pb), pb)].reshape(X * nb, pb)
    with scope("prod0"):
        sums_ref[...] = jnp.dot(weights(z, range(X), pl.ds(0, refs)), own_p, preferred_element_type=jnp.float32)

    for d in range(early, 1, -1):
        p_slot(d, 2)
        w_forwards(X - 1, d, None)
    p_slot(1, 3)
    w_forwards(X - 1, 1, None)

    @pl.loop(early + 1, Z)
    def _(d):
        for i in range(X):
            w_forwards(i, d, None)

    def near(fn, over):
        def at(src, right):
            ok = crosses(src) if over else jnp.logical_not(crosses(src))

            @pl.when(ok)
            def _():
                fn(src, right)
        sides(1, at)

    def lasts(d):
        for q in range(G):
            sides(d, last_step(q))

    near(second_step, False)

    @pl.loop(2, Z)
    def _(d):
        sides(d, second_step)

    near(add_step(range(X)), False)
    near(second_step, True)

    @pl.when(inner)
    def _():
        @pl.loop(2, Z)
        def _(d):
            sides(d, add_step(range(X)))

        near(add_step(range(X)), True)

    @pl.when(jnp.logical_not(inner))
    def _():
        @pl.loop(0, Z - 2)
        def _(e):
            sides(Z - 1 - e, add_step(range(max(X - 1, 1))))
            if X > 1:
                lasts(Z - 1 - e)

        if Z == 2:
            near(add_step(range(X)), True)

    with scope("drain"):
        for cp in started:
            cp.wait_send()
        for d in range(1, Z):
            p_copy(d).wait_send()

        def end_step(src, right):
            for cp in p_forward(src) + p_second(src):
                cp.wait_send()
            for i in range(X):
                @pl.when(forwards(src, right))
                def _():
                    for q in range(G):
                        w_go(i, src, q, right).wait_send()

        @pl.loop(1, Z)
        def _(d):
            sides(d, end_step)

        for i in range(X):
            for q in range(G):
                if Z > 2:
                    @pl.when(has_two)
                    def _():
                        w_two(i, q).wait_send()

                @pl.when(z < Z - 1)
                def _():
                    w_go(i, z, q, True).wait_send()

                @pl.when(z > 0)
                def _():
                    w_go(i, z, q, False).wait_send()


def flush_kernel(sums, evid, sums_out, evid_out, sem):
    n = sem.shape[0] - 1
    step = sums.shape[0] // n
    copies = [pltpu.make_async_copy(evid, evid_out, sem.at[n])]
    for i in range(n):
        part = pl.ds(i * step, step)
        copies.append(pltpu.make_async_copy(sums.at[part, :], sums_out.at[part, :], sem.at[i]))
    for cp in copies:
        cp.start()
    for cp in copies:
        cp.wait()


def exchange(mesh, images, templates, group_ids, group_ctf, group_prec, log_prior, class_mask):
    Z, X, C = mesh.shape["img"], mesh.shape["tpl"], mesh.shape["sub"]
    S = X * C
    rows, pix = images.shape
    refs = templates.shape[0]
    nb = C * rows
    pb = pix // Z
    H, G = PIECES, PARTS
    vmem = pl.BlockSpec(memory_space=pltpu.VMEM)
    anyw = pl.BlockSpec(memory_space=pl.ANY)
    dma = pltpu.SemaphoreType.DMA
    f32, bf16 = jnp.float32, jnp.bfloat16
    class_sums, evid = pl.pallas_call(
        functools.partial(exchange_kernel, (Z, X, C, H, G)),
        out_shape=(
            pltpu.VMEM((refs, pb), f32),
            pltpu.VMEM((1, rows), f32),
        ),
        in_specs=[anyw] * 7,
        out_specs=(vmem, vmem),
        scratch_shapes=[
            pltpu.VMEM((X, 1, nb), jnp.int32),
            pltpu.SMEM(group_ctf.shape, f32),
            pltpu.SMEM(group_prec.shape, f32),
            pltpu.SMEM(log_prior.shape, f32),
            pltpu.SMEM(class_mask.shape, jnp.int32),
            pltpu.VMEM((X, C, rows, pix), bf16),
            pltpu.VMEM((refs, pix), bf16),
            pltpu.VMEM((refs, nb), f32),
            pltpu.VMEM((refs, nb), f32),
            pltpu.VMEM((refs, nb), f32),
            pltpu.VMEM((X, Z, refs, nb), bf16),
            pltpu.VMEM((Z, X, C, rows, pb), bf16),
            pltpu.VMEM((X, 8, nb), f32),
            pltpu.VMEM((S, X, 8, nb), f32),
            pltpu.VMEM((Z, X, 8, nb), f32),
            dma((5,)), dma(()), dma(()), dma(()), dma((C,)), dma((X, H + C - 1)), dma((Z, X + C - 1)), dma((X, max(Z - 1, 1), G)), dma(()), dma((Z,)),
            pltpu.SemaphoreType.REGULAR((Z,)),
        ],
        compiler_params=pltpu.CompilerParams(
            collective_id=0, has_side_effects=True, vmem_limit_bytes=56 * 1024 * 1024
        ),
    )(group_ids.reshape(X, 1, nb), group_ctf, group_prec, log_prior, class_mask, images, templates)
    class_sums, evid = pl.pallas_call(
        flush_kernel,
        out_shape=(jax.ShapeDtypeStruct((refs, pb), f32), jax.ShapeDtypeStruct((1, rows), f32)),
        in_specs=[vmem, vmem],
        out_specs=(anyw, anyw),
        scratch_shapes=[dma((FLUSH + 1,))],
        compiler_params=pltpu.CompilerParams(vmem_limit_bytes=1024 * 1024),
    )(class_sums, evid)
    return class_sums, evid.reshape(rows)


def solution(mesh):
    placed = (
        P(("groups", "img", "tpl", "sub"), None),
        P(("groups", "tpl", "sub"), None),
        P(("groups", "img")),
        P("groups"),
        P("groups"),
        P("groups"),
        P("groups"),
    )
    return jax.shard_map(
        functools.partial(exchange, mesh),
        mesh=mesh,
        in_specs=placed,
        out_specs=(P(("groups", "tpl", "sub"), "img"), P(("groups", "img", "tpl", "sub"))),
        check_vma=False,
    )
```

```python
import functools
import jax
import jax.numpy as jnp
from jax import lax
from jax.experimental import pallas as pl
from jax.experimental.pallas import tpu as pltpu
from jax.sharding import PartitionSpec as P

ROTS = 16
MASKED = -1e30
PIECES = 4
PARTS = 4
NORM = 64
FLUSH = 4
MESH = pl.DeviceIdType.MESH


def exchange_kernel(
    sizes, ids_in, ctf_in, prec_in, prior_in, mask_in, images, templates,
    sums_ref, evid_ref,
    ids_ref, ctf_ref, prec_ref, prior_ref, mask_ref, grid_buf, tmpl, tnorm, base, act, all_w, all_p, own_stat, stat, fac,
    in_sem, tmpl_sem, own_sem, sent, c_recv, a_recv, p_recv, w_recv, s_recv, v_recv, up, side,
):
    Z, X, C, H, G = sizes
    S = X * C
    g, z, x, c = [lax.axis_index(n) for n in ("groups", "img", "tpl", "sub")]
    refs, nb = tnorm.shape
    classes = refs // ROTS
    rows, pix = grid_buf.shape[2:]
    pb = pix // Z
    hr = rows // H
    gr = refs // G
    s = x * C + c

    def chip(d):
        return lax.rem(x + d, X)

    def core(d):
        return lax.rem(c + d, C)

    def zoff(d):
        return lax.rem(z + d, Z)

    def dev(zz, xx, cc):
        return (g, zz, xx, cc)

    def scope(name):
        return jax.named_scope(name)

    peers = [(dx, dc) for dx in range(X) for dc in range(C) if dx or dc]
    inner = (z > 0) & (z < Z - 1)
    early = min(2, Z - 1)

    barrier = pltpu.get_barrier_semaphore()
    for dc in range(1, C):
        pl.semaphore_signal(barrier, inc=1, device_id=dev(z, x, core(dc)), device_id_type=MESH)

    @pl.loop(x + 1, X)
    def _(xx):
        for cc in range(C):
            pl.semaphore_signal(barrier, inc=1, device_id=dev(z, xx, cc), device_id_type=MESH)

    @pl.loop(z + 1, Z)
    def _(zz):
        pl.semaphore_signal(barrier, inc=1, device_id=dev(zz, x, c), device_id_type=MESH)

    started = []

    def local(src, dst, sem):
        cp = pltpu.make_async_copy(src, dst, sem)
        cp.start()
        return cp

    def copy(src, dst, send, recv, to):
        return pltpu.make_async_remote_copy(
            src_ref=src, dst_ref=dst, send_sem=send, recv_sem=recv, device_id=to, device_id_type=MESH
        )

    def remote(*args):
        cp = copy(*args)
        cp.start()
        started.append(cp)

    def arrive(dst, sem):
        pltpu.make_async_copy(dst, dst, sem).wait()

    small = [
        local(src, dst, in_sem.at[i])
        for i, (src, dst) in enumerate((
            (ids_in, ids_ref), (ctf_in, ctf_ref), (prec_in, prec_ref), (prior_in, prior_ref), (mask_in, mask_ref),
        ))
    ]
    tmpl_copy = local(templates, tmpl, tmpl_sem)
    own_copy = local(images, grid_buf.at[0, c], own_sem)

    with scope("barrier"):
        pl.semaphore_wait(barrier, C - 1 + x * C + z)

    @pl.loop(0, x)
    def _(xx):
        for cc in range(C):
            pl.semaphore_signal(side, inc=1, device_id=dev(z, xx, cc), device_id_type=MESH)

    @pl.loop(0, z)
    def _(zz):
        pl.semaphore_signal(up.at[z], inc=1, device_id=dev(zz, x, c), device_id_type=MESH)

    def piece(i, cc, h):
        return grid_buf.at[i, cc, pl.ds(h * hr, hr), :]

    for dc in range(1, C):
        remote(images, grid_buf.at[0, c], sent, c_recv.at[c], dev(z, x, core(dc)))
    def p_block(zz, i, cc):
        return all_p.at[zz, i, cc]

    def p_copy(d):
        zz = zoff(d)
        cols = pl.ds(pl.multiple_of(zz * pb, pb), pb)
        return copy(images.at[:, cols], p_block(z, 0, c), sent, p_recv.at[z, 0], dev(zz, x, c))

    def outer(d):
        zz = zoff(d)
        return (zz == 0) | (zz == Z - 1)

    def crosses(zz):
        return (2 * z < Z) != (2 * zz < Z)

    def p_send_inner(n):
        for d in range(1, Z):
            over = crosses(zoff(d)) & jnp.logical_not(inner)
            first = (z == 0) & (zoff(d) == 1)
            slot = jnp.where(over, 1, 0)

            @pl.when(jnp.logical_not(outer(d) | first) & (slot == n))
            def _():
                p_copy(d).start()

    for d in range(1, Z):
        @pl.when(zoff(d) == 0)
        def _():
            p_copy(d).start()

    with scope("side"):
        @pl.when(x < X - 1)
        def _():
            pl.semaphore_wait(side, (X - 1 - x) * C)
    for h in range(H):
        for dx in range(1, X):
            remote(
                images.at[pl.ds(h * hr, hr), :], piece(X - dx, c, h), sent, a_recv.at[X - dx, h],
                dev(z, chip(dx), c),
            )

    def p_far(first):
        @pl.loop(first, Z)
        def _(zz):
            pl.semaphore_wait(up.at[zz], 1)

        for d in range(1, Z):
            @pl.when(zoff(d) == Z - 1)
            def _():
                p_copy(d).start()

    with scope("up"):
        if Z > 2:
            @pl.when(z == 0)
            def _():
                pl.semaphore_wait(up.at[1], 1)
                p_copy(1).start()

            @pl.when(z > 0)
            def _():
                p_far(z + 1)

    with scope("small"):
        for cp in small:
            cp.wait()
    first = s * classes
    for i in range(classes):
        rws = pl.ds(i * ROTS, ROTS)
        base[rws, :] = jnp.full((ROTS, nb), prior_ref[first + i], jnp.float32)
        act[rws, :] = jnp.full((ROTS, nb), mask_ref[first + i], jnp.int32).astype(jnp.float32)

    factors, penalties = [], []
    for i in range(X):
        ids = ids_ref[chip(i)]
        ctf = jnp.zeros(ids.shape, jnp.float32)
        prec = ctf
        for q in range(ctf_ref.shape[0]):
            hit = ids == q
            ctf = jnp.where(hit, ctf_ref[q], ctf)
            prec = jnp.where(hit, prec_ref[q], prec)
        factors.append(prec * ctf)
        penalties.append(0.5 * prec * ctf * ctf)

    with scope("tmplw"):
        tmpl_copy.wait()

    with scope("tnorm"):
        @pl.loop(0, refs // NORM)
        def _(i):
            rws = pl.ds(pl.multiple_of(i * NORM, NORM), NORM)
            t = tmpl[rws, :].astype(jnp.float32)
            tnorm[rws, :] = jnp.broadcast_to(jnp.sum(t * t, axis=1, keepdims=True), (NORM, nb))

    def w_part(i, zz, q):
        return all_w.at[i, zz, pl.ds(q * gr, gr), :]

    def w_sem(i, src, dst, q):
        return w_recv.at[i, lax.rem(src - dst + Z - 1, Z), q]

    def w_go(i, zz, q, right):
        to = lax.rem(z + (1 if right else -1) + Z, Z)
        return copy(w_part(i, zz, q), w_part(i, zz, q), sent, w_sem(i, zz, to, q), dev(to, x, c))

    def w_two(i, q):
        zz = lax.rem(jnp.where(z == 0, z + 2, z - 2) + Z, Z)
        return copy(w_part(i, z, q), w_part(i, z, q), sent, w_sem(i, z, zz, q), dev(zz, x, c))

    has_two = ((z == 0) | (z == Z - 1)) if Z > 2 else None

    def forwards(src, right):
        if right:
            return (z < Z - 1) & ((src > 0) | (z != 1))
        return (z > 0) & ((src < Z - 1) | (z != Z - 2))

    def sides(d, fn):
        @pl.when(z - d >= 0)
        def _():
            fn(z - d, True)

        @pl.when(z + d < Z)
        def _():
            fn(z + d, False)

    def w_forward(i, q):
        def fn(src, right):
            @pl.when(forwards(src, right))
            def _():
                with scope(f"wf{i}"):
                    arrive(w_part(i, src, q), w_sem(i, src, z, q))
                w_go(i, src, q, right).start()
        return fn

    def w_forwards(i, d, side, parts=range(G)):
        def fn(src, right):
            if side is None or side == right:
                for q in parts:
                    w_forward(i, q)(src, right)
        sides(d, fn)

    def w_wait(i, q):
        def fn(src, right):
            @pl.when(jnp.logical_not(forwards(src, right)))
            def _():
                with scope(f"ww{i}"):
                    arrive(w_part(i, src, q), w_sem(i, src, z, q))
        return fn

    def scores(i):
        pixels = grid_buf[i].reshape(nb, pix)
        raw = lax.dot_general(pixels, tmpl[...], (((1,), (1,)), ((), ())), preferred_element_type=jnp.float32).T
        live = act[...] > 0.0
        values = jnp.where(live, factors[i] * raw - penalties[i] * tnorm[...] + base[...], MASKED)
        peak = jnp.max(values, axis=0, keepdims=True)
        terms = jnp.where(live, jnp.exp(values - peak), 0.0)
        all_w[i, z] = terms.astype(jnp.bfloat16)
        total = jnp.sum(terms, axis=0, keepdims=True)
        row = lax.broadcasted_iota(jnp.int32, (8, nb), 0)
        own_stat[chip(i)] = jnp.where(row == 0, peak, total)

    def w_start(i):
        if Z > 2:
            @pl.when(has_two)
            def _():
                for q in range(G):
                    w_two(i, q).start()

        for q in range(G):
            @pl.when(z < Z - 1)
            def _():
                w_go(i, z, q, True).start()

            @pl.when(z > 0)
            def _():
                w_go(i, z, q, False).start()

    def p_forward(zz):
        out = []
        for dx in range(1, X):
            out.append(copy(p_block(zz, 0, c), p_block(zz, X - dx, c), sent, p_recv.at[zz, X - dx], dev(z, chip(dx), c)))
        for dc in range(1, C):
            out.append(copy(p_block(zz, 0, c), p_block(zz, 0, c), sent, p_recv.at[zz, X + C - 1 - dc], dev(z, x, core(dc))))
        return out

    def p_second(zz):
        out = []
        for dx in range(1, X):
            for dc in range(1, C):
                out.append(copy(p_block(zz, dx, c), p_block(zz, dx, c), sent, p_recv.at[zz, X + C - 1 - dc], dev(z, x, core(dc))))
        return out

    def p_start(zz, right):
        with scope("pst"):
            arrive(p_block(zz, 0, c), p_recv.at[zz, 0])
        for cp in p_forward(zz):
            cp.start()

    def p_slot(d, n):
        def fn(src, right):
            far = 3 if d == 1 else 2
            slot = jnp.where(inner & crosses(src), far, jnp.where(inner | (d == 1), 0, 1))

            @pl.when(slot == n)
            def _():
                p_start(src, right)
        sides(d, fn)

    def gather(dx, h):
        with scope(f"gath{h}"):
            arrive(piece(dx, c, h), a_recv.at[dx, h])
        for dc in range(1, C):
            remote(piece(dx, c, h), piece(dx, c, h), sent, a_recv.at[dx, H + C - 1 - dc], dev(z, x, core(dc)))

    own_copy.wait()
    with scope("own"):
        for dc in range(1, C):
            arrive(grid_buf.at[0, core(dc)], c_recv.at[core(dc)])
    with scope("sc0"):
        scores(0)

    @pl.when(z == 0)
    def _():
        p_far(min(2, Z - 1))

    w_start(0)
    if X == 1:
        p_send_inner(1)
    p_send_inner(0)

    for dx in range(1, X):
        for h in range(H // 2):
            gather(dx, h)
        for d in range(early, 1, -1):
            w_forwards(dx - 1, d, False)
        for h in range(H // 2, H - 1):
            gather(dx, h)
        for d in range(early, 1, -1):
            w_forwards(dx - 1, d, True, range(G - 1))
        w_forwards(dx - 1, 1, False, range(G // 2))
        gather(dx, H - 1)
        for d in range(early, 1, -1):
            w_forwards(dx - 1, d, True, range(G - 1, G))
        w_forwards(dx - 1, 1, False, range(G // 2, G))
        if dx == X - 1:
            p_send_inner(1)
            for d in range(1, early + 1):
                p_slot(d, 0)
        with scope(f"arrA{dx}"):
            for dc in range(1, C):
                arrive(grid_buf.at[dx, core(dc)], a_recv.at[dx, H + dc - 1])
        with scope(f"sc{dx}"):
            scores(dx)
        w_start(dx)

    for dx, dc in peers:
        remote(own_stat, stat.at[s], sent, s_recv, dev(z, chip(dx), core(dc)))

    for i in range(X - 1):
        w_forwards(i, 1, True)
    for d in range(1, early + 1):
        p_slot(d, 1)

    @pl.loop(early + 1, Z)
    def _(d):
        sides(d, p_start)

    with scope("stat"):
        arrive(stat.at[pl.ds(0, S - 1)], s_recv)
    for i in range(X):
        xs = chip(i)
        own = own_stat[xs]
        parts = [(own[0:1], own[1:2])]
        for dx, dc in peers:
            got = stat[chip(dx) * C + core(dc), xs]
            parts.append((got[0:1], got[1:2]))
        peak = functools.reduce(jnp.maximum, [p for p, _ in parts])
        total = functools.reduce(jnp.add, [t * jnp.exp(p - peak) for p, t in parts])
        fac[z, i] = jnp.broadcast_to(factors[i] * jnp.exp(own[0:1] - peak) / total, (8, nb))
        if i == 0:
            evid = peak + jnp.log(total)
            mine = evid[:, 0:rows]
            for q in range(1, C):
                mine = jnp.where(c == q, evid[:, q * rows : (q + 1) * rows], mine)
            evid_ref[...] = mine
    for d in range(1, Z):
        remote(fac.at[z], fac.at[z], sent, v_recv.at[z], dev(zoff(d), x, c))

    def near(fn, over):
        def at(src, right):
            ok = crosses(src) if over else jnp.logical_not(crosses(src))

            @pl.when(ok)
            def _():
                fn(src, right)
        sides(1, at)

    def second_step(src, right):
        for dx in range(1, X):
            with scope("psec"):
                arrive(p_block(src, dx, c), p_recv.at[src, dx])
        for cp in p_second(src):
            cp.start()

    def weights(zz, chunks, rws):
        return jnp.concatenate(
            [(all_w[i, zz, rws, :].astype(jnp.float32) * fac[zz, i, 0:1]).astype(jnp.bfloat16) for i in chunks], axis=1
        )

    def product(zz, chunks, rws):
        block = all_p[zz, chunks[0] : chunks[-1] + 1].reshape(len(chunks) * nb, pb)
        sums_ref[rws, :] += jnp.dot(weights(zz, chunks, rws), block, preferred_element_type=jnp.float32)

    def add_step(chunks):
        def fn(src, right):
            for i in chunks:
                for q in range(G):
                    w_wait(i, q)(src, right)
            with scope("vw"):
                arrive(fac.at[src], v_recv.at[src])
            with scope("addw"):
                for dc in range(1, C):
                    arrive(all_p.at[src, :, core(dc)], p_recv.at[src, X + dc - 1])
            with scope("addp"):
                product(src, chunks, pl.ds(0, refs))
        return fn

    def last_step(q):
        def fn(src, right):
            w_wait(X - 1, q)(src, right)
            with scope(f"last{q}"):
                product(src, range(X - 1, X), pl.ds(q * gr, gr))
        return fn

    own_p = grid_buf[:, :, :, pl.ds(pl.multiple_of(z * pb, pb), pb)].reshape(X * nb, pb)
    with scope("prod0"):
        sums_ref[...] = jnp.dot(weights(z, range(X), pl.ds(0, refs)), own_p, preferred_element_type=jnp.float32)

    near(second_step, False)

    for d in range(early, 1, -1):
        p_slot(d, 2)
        w_forwards(X - 1, d, None)
    p_slot(1, 3)
    w_forwards(X - 1, 1, None)

    @pl.loop(early + 1, Z)
    def _(d):
        for i in range(X):
            w_forwards(i, d, None)

    def lasts(d):
        for q in range(G):
            sides(d, last_step(q))

    @pl.loop(2, Z)
    def _(d):
        sides(d, second_step)

    near(add_step(range(X)), False)
    near(second_step, True)

    @pl.when(inner)
    def _():
        @pl.loop(2, Z)
        def _(d):
            sides(d, add_step(range(X)))

        near(add_step(range(X)), True)

    @pl.when(jnp.logical_not(inner))
    def _():
        @pl.loop(3, Z)
        def _(d):
            sides(d, add_step(range(X)))

        if Z > 2:
            sides(2, add_step(range(max(X - 1, 1))))
            if X > 1:
                lasts(2)
        else:
            near(add_step(range(X)), True)

    with scope("drain"):
        for cp in started:
            cp.wait_send()
        for d in range(1, Z):
            p_copy(d).wait_send()

        def end_step(src, right):
            for cp in p_forward(src) + p_second(src):
                cp.wait_send()
            for i in range(X):
                @pl.when(forwards(src, right))
                def _():
                    for q in range(G):
                        w_go(i, src, q, right).wait_send()

        @pl.loop(1, Z)
        def _(d):
            sides(d, end_step)

        for i in range(X):
            for q in range(G):
                if Z > 2:
                    @pl.when(has_two)
                    def _():
                        w_two(i, q).wait_send()

                @pl.when(z < Z - 1)
                def _():
                    w_go(i, z, q, True).wait_send()

                @pl.when(z > 0)
                def _():
                    w_go(i, z, q, False).wait_send()


def flush_kernel(sums, evid, sums_out, evid_out, sem):
    n = sem.shape[0] - 1
    step = sums.shape[0] // n
    copies = [pltpu.make_async_copy(evid, evid_out, sem.at[n])]
    for i in range(n):
        part = pl.ds(i * step, step)
        copies.append(pltpu.make_async_copy(sums.at[part, :], sums_out.at[part, :], sem.at[i]))
    for cp in copies:
        cp.start()
    for cp in copies:
        cp.wait()


def exchange(mesh, images, templates, group_ids, group_ctf, group_prec, log_prior, class_mask):
    Z, X, C = mesh.shape["img"], mesh.shape["tpl"], mesh.shape["sub"]
    S = X * C
    rows, pix = images.shape
    refs = templates.shape[0]
    nb = C * rows
    pb = pix // Z
    H, G = PIECES, PARTS
    vmem = pl.BlockSpec(memory_space=pltpu.VMEM)
    anyw = pl.BlockSpec(memory_space=pl.ANY)
    dma = pltpu.SemaphoreType.DMA
    f32, bf16 = jnp.float32, jnp.bfloat16
    class_sums, evid = pl.pallas_call(
        functools.partial(exchange_kernel, (Z, X, C, H, G)),
        out_shape=(
            pltpu.VMEM((refs, pb), f32),
            pltpu.VMEM((1, rows), f32),
        ),
        in_specs=[anyw] * 7,
        out_specs=(vmem, vmem),
        scratch_shapes=[
            pltpu.VMEM((X, 1, nb), jnp.int32),
            pltpu.SMEM(group_ctf.shape, f32),
            pltpu.SMEM(group_prec.shape, f32),
            pltpu.SMEM(log_prior.shape, f32),
            pltpu.SMEM(class_mask.shape, jnp.int32),
            pltpu.VMEM((X, C, rows, pix), bf16),
            pltpu.VMEM((refs, pix), bf16),
            pltpu.VMEM((refs, nb), f32),
            pltpu.VMEM((refs, nb), f32),
            pltpu.VMEM((refs, nb), f32),
            pltpu.VMEM((X, Z, refs, nb), bf16),
            pltpu.VMEM((Z, X, C, rows, pb), bf16),
            pltpu.VMEM((X, 8, nb), f32),
            pltpu.VMEM((S, X, 8, nb), f32),
            pltpu.VMEM((Z, X, 8, nb), f32),
            dma((5,)), dma(()), dma(()), dma(()), dma((C,)), dma((X, H + C - 1)), dma((Z, X + C - 1)), dma((X, max(Z - 1, 1), G)), dma(()), dma((Z,)),
            pltpu.SemaphoreType.REGULAR((Z,)), pltpu.SemaphoreType.REGULAR,
        ],
        compiler_params=pltpu.CompilerParams(
            collective_id=0, has_side_effects=True, vmem_limit_bytes=56 * 1024 * 1024
        ),
    )(group_ids.reshape(X, 1, nb), group_ctf, group_prec, log_prior, class_mask, images, templates)
    class_sums, evid = pl.pallas_call(
        flush_kernel,
        out_shape=(jax.ShapeDtypeStruct((refs, pb), f32), jax.ShapeDtypeStruct((1, rows), f32)),
        in_specs=[vmem, vmem],
        out_specs=(anyw, anyw),
        scratch_shapes=[dma((FLUSH + 1,))],
        compiler_params=pltpu.CompilerParams(vmem_limit_bytes=1024 * 1024),
    )(class_sums, evid)
    return class_sums, evid.reshape(rows)


def solution(mesh):
    placed = (
        P(("groups", "img", "tpl", "sub"), None),
        P(("groups", "tpl", "sub"), None),
        P(("groups", "img")),
        P("groups"),
        P("groups"),
        P("groups"),
        P("groups"),
    )
    return jax.shard_map(
        functools.partial(exchange, mesh),
        mesh=mesh,
        in_specs=placed,
        out_specs=(P(("groups", "tpl", "sub"), "img"), P(("groups", "img", "tpl", "sub"))),
        check_vma=False,
    )
```

```python
import functools
import jax
import jax.numpy as jnp
from jax import lax
from jax.experimental import pallas as pl
from jax.experimental.pallas import tpu as pltpu
from jax.sharding import PartitionSpec as P

ROTS = 16
MASKED = -1e30
PIECES = 4
PARTS = 4
LAST_PARTS = 8
NORM = 64
FLUSH = 4
MESH = pl.DeviceIdType.MESH


def exchange_kernel(
    sizes, ids_in, ctf_in, prec_in, prior_in, mask_in, images, templates,
    sums_ref, evid_ref,
    ids_ref, ctf_ref, prec_ref, prior_ref, mask_ref, grid_buf, tmpl, tnorm, base, act, all_w, all_p, own_stat, stat, fac,
    in_sem, tmpl_sem, own_sem, sent, c_recv, a_recv, p_recv, w_recv, s_recv, v_recv, up, side,
):
    Z, X, C, H, G, GL = sizes
    S = X * C
    g, z, x, c = [lax.axis_index(n) for n in ("groups", "img", "tpl", "sub")]
    refs, nb = tnorm.shape
    classes = refs // ROTS
    rows, pix = grid_buf.shape[2:]
    pb = pix // Z
    hr = rows // H
    s = x * C + c

    def chip(d):
        return lax.rem(x + d, X)

    def core(d):
        return lax.rem(c + d, C)

    def zoff(d):
        return lax.rem(z + d, Z)

    def dev(zz, xx, cc):
        return (g, zz, xx, cc)

    def hop(src, dst):
        return lax.rem(src - dst + Z - 1, Z)

    def scope(name):
        return jax.named_scope(name)

    peers = [(dx, dc) for dx in range(X) for dc in range(C) if dx or dc]
    inner = (z > 0) & (z < Z - 1)
    early = min(2, Z - 1)

    barrier = pltpu.get_barrier_semaphore()
    for dc in range(1, C):
        pl.semaphore_signal(barrier, inc=1, device_id=dev(z, x, core(dc)), device_id_type=MESH)

    @pl.loop(x + 1, X)
    def _(xx):
        for cc in range(C):
            pl.semaphore_signal(barrier, inc=1, device_id=dev(z, xx, cc), device_id_type=MESH)

    @pl.loop(z + 1, Z)
    def _(zz):
        pl.semaphore_signal(barrier, inc=1, device_id=dev(zz, x, c), device_id_type=MESH)

    started = []

    def local(src, dst, sem):
        cp = pltpu.make_async_copy(src, dst, sem)
        cp.start()
        return cp

    def copy(src, dst, send, recv, to):
        return pltpu.make_async_remote_copy(
            src_ref=src, dst_ref=dst, send_sem=send, recv_sem=recv, device_id=to, device_id_type=MESH
        )

    def remote(*args):
        cp = copy(*args)
        cp.start()
        started.append(cp)

    def arrive(dst, sem):
        pltpu.make_async_copy(dst, dst, sem).wait()

    small = [
        local(src, dst, in_sem.at[i])
        for i, (src, dst) in enumerate((
            (ids_in, ids_ref), (ctf_in, ctf_ref), (prec_in, prec_ref), (prior_in, prior_ref), (mask_in, mask_ref),
        ))
    ]
    tmpl_copy = local(templates, tmpl, tmpl_sem)
    own_copy = local(images, grid_buf.at[0, c], own_sem)

    with scope("barrier"):
        pl.semaphore_wait(barrier, C - 1 + x * C + z)

    @pl.loop(0, x)
    def _(xx):
        for cc in range(C):
            pl.semaphore_signal(side, inc=1, device_id=dev(z, xx, cc), device_id_type=MESH)

    @pl.loop(0, z)
    def _(zz):
        pl.semaphore_signal(up.at[jnp.where(zz == z - 1, 0, 1)], inc=1, device_id=dev(zz, x, c), device_id_type=MESH)

    def piece(i, cc, h):
        return grid_buf.at[i, cc, pl.ds(h * hr, hr), :]

    for dc in range(1, C):
        remote(images, grid_buf.at[0, c], sent, c_recv.at[C - dc - 1], dev(z, x, core(dc)))
    def p_block(zz, i, cc):
        return all_p.at[zz, i, cc]

    def p_copy(d):
        zz = zoff(d)
        cols = pl.ds(pl.multiple_of(zz * pb, pb), pb)
        return copy(images.at[:, cols], p_block(z, 0, c), sent, p_recv.at[hop(z, zz), 0], dev(zz, x, c))

    def outer(d):
        zz = zoff(d)
        return (zz == 0) | (zz == Z - 1)

    def crosses(zz):
        return (2 * z < Z) != (2 * zz < Z)

    def p_send_inner(n):
        for d in range(1, Z):
            over = crosses(zoff(d)) & jnp.logical_not(inner)
            first = (z == 0) & (zoff(d) == 1)
            slot = jnp.where(over, 1, 0)

            @pl.when(jnp.logical_not(outer(d) | first) & (slot == n))
            def _():
                p_copy(d).start()

    for d in range(1, Z):
        @pl.when(zoff(d) == 0)
        def _():
            p_copy(d).start()

    with scope("side"):
        @pl.when(x < X - 1)
        def _():
            pl.semaphore_wait(side, (X - 1 - x) * C)
    for h in range(H):
        for dx in range(1, X):
            remote(
                images.at[pl.ds(h * hr, hr), :], piece(X - dx, c, h), sent, a_recv.at[X - dx - 1, h],
                dev(z, chip(dx), c),
            )

    def wait_next():
        @pl.when(z < Z - 1)
        def _():
            pl.semaphore_wait(up.at[0], 1)

    def p_far():
        @pl.when(z < Z - 2)
        def _():
            pl.semaphore_wait(up.at[1], Z - 2 - z)

        for d in range(1, Z):
            @pl.when(zoff(d) == Z - 1)
            def _():
                p_copy(d).start()

    with scope("up"):
        if Z > 2:
            @pl.when(z == 0)
            def _():
                wait_next()
                p_copy(1).start()

            @pl.when(z > 0)
            def _():
                wait_next()
                p_far()

    with scope("small"):
        for cp in small:
            cp.wait()
    first = s * classes
    for i in range(classes):
        rws = pl.ds(i * ROTS, ROTS)
        base[rws, :] = jnp.full((ROTS, nb), prior_ref[first + i], jnp.float32)
        act[rws, :] = jnp.full((ROTS, nb), mask_ref[first + i], jnp.int32).astype(jnp.float32)

    factors, penalties = [], []
    for i in range(X):
        ids = ids_ref[chip(i)]
        ctf = jnp.zeros(ids.shape, jnp.float32)
        prec = ctf
        for q in range(ctf_ref.shape[0]):
            hit = ids == q
            ctf = jnp.where(hit, ctf_ref[q], ctf)
            prec = jnp.where(hit, prec_ref[q], prec)
        factors.append(prec * ctf)
        penalties.append(0.5 * prec * ctf * ctf)

    with scope("tmplw"):
        tmpl_copy.wait()

    with scope("tnorm"):
        @pl.loop(0, refs // NORM)
        def _(i):
            rws = pl.ds(pl.multiple_of(i * NORM, NORM), NORM)
            t = tmpl[rws, :].astype(jnp.float32)
            tnorm[rws, :] = jnp.broadcast_to(jnp.sum(t * t, axis=1, keepdims=True), (NORM, nb))

    def count(i):
        return GL if i == X - 1 else G

    def w_part(i, zz, q):
        n = refs // count(i)
        return all_w.at[i, zz, pl.ds(q * n, n), :]

    def w_sem(i, src, dst, q):
        return w_recv.at[hop(src, dst), i * G + q]

    def w_go(i, zz, q, right):
        to = lax.rem(z + (1 if right else -1) + Z, Z)
        return copy(w_part(i, zz, q), w_part(i, zz, q), sent, w_sem(i, zz, to, q), dev(to, x, c))

    def w_two(i, q):
        zz = lax.rem(jnp.where(z == 0, z + 2, z - 2) + Z, Z)
        return copy(w_part(i, z, q), w_part(i, z, q), sent, w_sem(i, z, zz, q), dev(zz, x, c))

    has_two = ((z == 0) | (z == Z - 1)) if Z > 2 else None

    def forwards(src, right):
        if right:
            return (z < Z - 1) & ((src > 0) | (z != 1))
        return (z > 0) & ((src < Z - 1) | (z != Z - 2))

    def sides(d, fn):
        @pl.when(z - d >= 0)
        def _():
            fn(z - d, True)

        @pl.when(z + d < Z)
        def _():
            fn(z + d, False)

    def w_forward(i, q):
        def fn(src, right):
            @pl.when(forwards(src, right))
            def _():
                with scope(f"wf{i}"):
                    arrive(w_part(i, src, q), w_sem(i, src, z, q))
                w_go(i, src, q, right).start()
        return fn

    def w_forwards(i, d, side, parts=None):
        def fn(src, right):
            if side is None or side == right:
                for q in parts or range(count(i)):
                    w_forward(i, q)(src, right)
        sides(d, fn)

    def w_wait(i, q):
        def fn(src, right):
            @pl.when(jnp.logical_not(forwards(src, right)))
            def _():
                with scope(f"ww{i}"):
                    arrive(w_part(i, src, q), w_sem(i, src, z, q))
        return fn

    def scores(i):
        pixels = grid_buf[i].reshape(nb, pix)
        raw = lax.dot_general(pixels, tmpl[...], (((1,), (1,)), ((), ())), preferred_element_type=jnp.float32).T
        live = act[...] > 0.0
        values = jnp.where(live, factors[i] * raw - penalties[i] * tnorm[...] + base[...], MASKED)
        peak = jnp.max(values, axis=0, keepdims=True)
        terms = jnp.where(live, jnp.exp(values - peak), 0.0)
        all_w[i, z] = terms.astype(jnp.bfloat16)
        total = jnp.sum(terms, axis=0, keepdims=True)
        row = lax.broadcasted_iota(jnp.int32, (8, nb), 0)
        own_stat[chip(i)] = jnp.where(row == 0, peak, total)

    def w_start(i):
        if Z > 2:
            @pl.when(has_two)
            def _():
                for q in range(count(i)):
                    w_two(i, q).start()

        for q in range(count(i)):
            @pl.when(z < Z - 1)
            def _():
                w_go(i, z, q, True).start()

            @pl.when(z > 0)
            def _():
                w_go(i, z, q, False).start()

    def p_forward(zz):
        out = []
        for dx in range(1, X):
            out.append(copy(p_block(zz, 0, c), p_block(zz, X - dx, c), sent, p_recv.at[hop(zz, z), X - dx], dev(z, chip(dx), c)))
        for dc in range(1, C):
            out.append(copy(p_block(zz, 0, c), p_block(zz, 0, c), sent, p_recv.at[hop(zz, z), X + C - 1 - dc], dev(z, x, core(dc))))
        return out

    def p_second(zz):
        out = []
        for dx in range(1, X):
            for dc in range(1, C):
                out.append(copy(p_block(zz, dx, c), p_block(zz, dx, c), sent, p_recv.at[hop(zz, z), X + C - 1 - dc], dev(z, x, core(dc))))
        return out

    def p_start(zz, right):
        with scope("pst"):
            arrive(p_block(zz, 0, c), p_recv.at[hop(zz, z), 0])
        for cp in p_forward(zz):
            cp.start()

    def p_slot(d, n):
        def fn(src, right):
            far = 3 if d == 1 else 2
            slot = jnp.where(inner & crosses(src), far, jnp.where(inner | (d == 1), 0, 1))

            @pl.when(slot == n)
            def _():
                p_start(src, right)
        sides(d, fn)

    def gather(dx, h):
        with scope(f"gath{h}"):
            arrive(piece(dx, c, h), a_recv.at[dx - 1, h])
        for dc in range(1, C):
            remote(piece(dx, c, h), piece(dx, c, h), sent, a_recv.at[dx - 1, H + C - 1 - dc], dev(z, x, core(dc)))

    own_copy.wait()
    with scope("own"):
        for dc in range(1, C):
            arrive(grid_buf.at[0, core(dc)], c_recv.at[dc - 1])
    with scope("sc0"):
        scores(0)

    @pl.when(z == 0)
    def _():
        if Z == 2:
            wait_next()
        p_far()

    w_start(0)
    if X == 1:
        p_send_inner(1)
    p_send_inner(0)

    for dx in range(1, X):
        for h in range(H // 2):
            gather(dx, h)
        for d in range(early, 1, -1):
            w_forwards(dx - 1, d, False)
        for h in range(H // 2, H - 1):
            gather(dx, h)
        for d in range(early, 1, -1):
            w_forwards(dx - 1, d, True, range(G - 1))
        w_forwards(dx - 1, 1, False, range(G // 2))
        gather(dx, H - 1)
        for d in range(early, 1, -1):
            w_forwards(dx - 1, d, True, range(G - 1, G))
        w_forwards(dx - 1, 1, False, range(G // 2, G))
        if dx == X - 1:
            p_send_inner(1)
            for d in range(1, early + 1):
                p_slot(d, 0)
        with scope(f"arrA{dx}"):
            for dc in range(1, C):
                arrive(grid_buf.at[dx, core(dc)], a_recv.at[dx - 1, H + dc - 1])
        with scope(f"sc{dx}"):
            scores(dx)
        w_start(dx)

    for dx, dc in peers:
        remote(own_stat, stat.at[s], sent, s_recv, dev(z, chip(dx), core(dc)))

    for i in range(X - 1):
        w_forwards(i, 1, True)
    for d in range(1, early + 1):
        p_slot(d, 1)

    @pl.loop(early + 1, Z)
    def _(d):
        sides(d, p_start)

    with scope("stat"):
        arrive(stat.at[pl.ds(0, S - 1)], s_recv)
    for i in range(X):
        xs = chip(i)
        own = own_stat[xs]
        parts = [(own[0:1], own[1:2])]
        for dx, dc in peers:
            got = stat[chip(dx) * C + core(dc), xs]
            parts.append((got[0:1], got[1:2]))
        peak = functools.reduce(jnp.maximum, [p for p, _ in parts])
        total = functools.reduce(jnp.add, [t * jnp.exp(p - peak) for p, t in parts])
        fac[z, i] = jnp.broadcast_to(factors[i] * jnp.exp(own[0:1] - peak) / total, (8, nb))
        if i == 0:
            evid = peak + jnp.log(total)
            mine = evid[:, 0:rows]
            for q in range(1, C):
                mine = jnp.where(c == q, evid[:, q * rows : (q + 1) * rows], mine)
            evid_ref[...] = mine
    for d in range(1, Z):
        remote(fac.at[z], fac.at[z], sent, v_recv.at[Z - d - 1], dev(zoff(d), x, c))

    def near(fn, over):
        def at(src, right):
            ok = crosses(src) if over else jnp.logical_not(crosses(src))

            @pl.when(ok)
            def _():
                fn(src, right)
        sides(1, at)

    def second_step(src, right):
        for dx in range(1, X):
            with scope("psec"):
                arrive(p_block(src, dx, c), p_recv.at[hop(src, z), dx])
        for cp in p_second(src):
            cp.start()

    def weights(zz, chunks, rws):
        return jnp.concatenate(
            [(all_w[i, zz, rws, :].astype(jnp.float32) * fac[zz, i, 0:1]).astype(jnp.bfloat16) for i in chunks], axis=1
        )

    def product(zz, chunks, rws):
        block = all_p[zz, chunks[0] : chunks[-1] + 1].reshape(len(chunks) * nb, pb)
        sums_ref[rws, :] += jnp.dot(weights(zz, chunks, rws), block, preferred_element_type=jnp.float32)

    def add_step(chunks):
        def fn(src, right):
            for i in chunks:
                for q in range(count(i)):
                    w_wait(i, q)(src, right)
            with scope("vw"):
                arrive(fac.at[src], v_recv.at[hop(src, z)])
            with scope("addw"):
                for dc in range(1, C):
                    arrive(all_p.at[src, :, core(dc)], p_recv.at[hop(src, z), X + dc - 1])
            with scope("addp"):
                product(src, chunks, pl.ds(0, refs))
        return fn

    def last_step(q):
        def fn(src, right):
            w_wait(X - 1, q)(src, right)
            with scope(f"last{q}"):
                product(src, range(X - 1, X), pl.ds(q * (refs // GL), refs // GL))
        return fn

    own_p = grid_buf[:, :, :, pl.ds(pl.multiple_of(z * pb, pb), pb)].reshape(X * nb, pb)
    with scope("prod0"):
        sums_ref[...] = jnp.dot(weights(z, range(X), pl.ds(0, refs)), own_p, preferred_element_type=jnp.float32)

    near(second_step, False)

    for d in range(early, 1, -1):
        p_slot(d, 2)
        w_forwards(X - 1, d, None)
    p_slot(1, 3)
    w_forwards(X - 1, 1, None)

    @pl.loop(early + 1, Z)
    def _(d):
        for i in range(X):
            w_forwards(i, d, None)

    def lasts(d):
        for q in range(GL):
            sides(d, last_step(q))

    @pl.loop(2, Z)
    def _(d):
        sides(d, second_step)

    near(add_step(range(X)), False)
    near(second_step, True)

    @pl.when(inner)
    def _():
        @pl.loop(2, Z)
        def _(d):
            sides(d, add_step(range(X)))

        near(add_step(range(X)), True)

    @pl.when(jnp.logical_not(inner))
    def _():
        @pl.loop(3, Z)
        def _(d):
            sides(d, add_step(range(X)))

        if Z > 2:
            sides(2, add_step(range(max(X - 1, 1))))
            if X > 1:
                lasts(2)
        else:
            near(add_step(range(X)), True)

    with scope("drain"):
        for cp in started:
            cp.wait_send()
        for d in range(1, Z):
            p_copy(d).wait_send()

        def end_step(src, right):
            for cp in p_forward(src) + p_second(src):
                cp.wait_send()
            for i in range(X):
                @pl.when(forwards(src, right))
                def _():
                    for q in range(count(i)):
                        w_go(i, src, q, right).wait_send()

        @pl.loop(1, Z)
        def _(d):
            sides(d, end_step)

        for i in range(X):
            for q in range(count(i)):
                if Z > 2:
                    @pl.when(has_two)
                    def _():
                        w_two(i, q).wait_send()

                @pl.when(z < Z - 1)
                def _():
                    w_go(i, z, q, True).wait_send()

                @pl.when(z > 0)
                def _():
                    w_go(i, z, q, False).wait_send()


def flush_kernel(sums, evid, sums_out, evid_out, sem):
    n = sem.shape[0] - 1
    step = sums.shape[0] // n
    copies = [pltpu.make_async_copy(evid, evid_out, sem.at[n])]
    for i in range(n):
        part = pl.ds(i * step, step)
        copies.append(pltpu.make_async_copy(sums.at[part, :], sums_out.at[part, :], sem.at[i]))
    for cp in copies:
        cp.start()
    for cp in copies:
        cp.wait()


def exchange(mesh, images, templates, group_ids, group_ctf, group_prec, log_prior, class_mask):
    Z, X, C = mesh.shape["img"], mesh.shape["tpl"], mesh.shape["sub"]
    S = X * C
    rows, pix = images.shape
    refs = templates.shape[0]
    nb = C * rows
    pb = pix // Z
    H, G, GL = PIECES, PARTS, LAST_PARTS
    vmem = pl.BlockSpec(memory_space=pltpu.VMEM)
    anyw = pl.BlockSpec(memory_space=pl.ANY)
    dma = pltpu.SemaphoreType.DMA
    f32, bf16 = jnp.float32, jnp.bfloat16
    class_sums, evid = pl.pallas_call(
        functools.partial(exchange_kernel, (Z, X, C, H, G, GL)),
        out_shape=(
            pltpu.VMEM((refs, pb), f32),
            pltpu.VMEM((1, rows), f32),
        ),
        in_specs=[anyw] * 7,
        out_specs=(vmem, vmem),
        scratch_shapes=[
            pltpu.VMEM((X, 1, nb), jnp.int32),
            pltpu.SMEM(group_ctf.shape, f32),
            pltpu.SMEM(group_prec.shape, f32),
            pltpu.SMEM(log_prior.shape, f32),
            pltpu.SMEM(class_mask.shape, jnp.int32),
            pltpu.VMEM((X, C, rows, pix), bf16),
            pltpu.VMEM((refs, pix), bf16),
            pltpu.VMEM((refs, nb), f32),
            pltpu.VMEM((refs, nb), f32),
            pltpu.VMEM((refs, nb), f32),
            pltpu.VMEM((X, Z, refs, nb), bf16),
            pltpu.VMEM((Z, X, C, rows, pb), bf16),
            pltpu.VMEM((X, 8, nb), f32),
            pltpu.VMEM((S, X, 8, nb), f32),
            pltpu.VMEM((Z, X, 8, nb), f32),
            dma((5,)), dma(()), dma(()), dma(()), dma((max(C - 1, 1),)), dma((max(X - 1, 1), H + C - 1)), dma((max(Z - 1, 1), X + C - 1)), dma((max(Z - 1, 1), (X - 1) * G + GL)), dma(()), dma((max(Z - 1, 1),)),
            pltpu.SemaphoreType.REGULAR((2,)), pltpu.SemaphoreType.REGULAR,
        ],
        compiler_params=pltpu.CompilerParams(
            collective_id=0, has_side_effects=True, vmem_limit_bytes=56 * 1024 * 1024
        ),
    )(group_ids.reshape(X, 1, nb), group_ctf, group_prec, log_prior, class_mask, images, templates)
    class_sums, evid = pl.pallas_call(
        flush_kernel,
        out_shape=(jax.ShapeDtypeStruct((refs, pb), f32), jax.ShapeDtypeStruct((1, rows), f32)),
        in_specs=[vmem, vmem],
        out_specs=(anyw, anyw),
        scratch_shapes=[dma((FLUSH + 1,))],
        compiler_params=pltpu.CompilerParams(vmem_limit_bytes=1024 * 1024),
    )(class_sums, evid)
    return class_sums, evid.reshape(rows)


def solution(mesh):
    placed = (
        P(("groups", "img", "tpl", "sub"), None),
        P(("groups", "tpl", "sub"), None),
        P(("groups", "img")),
        P("groups"),
        P("groups"),
        P("groups"),
        P("groups"),
    )
    return jax.shard_map(
        functools.partial(exchange, mesh),
        mesh=mesh,
        in_specs=placed,
        out_specs=(P(("groups", "tpl", "sub"), "img"), P(("groups", "img", "tpl", "sub"))),
        check_vma=False,
    )
```

```python
import functools
import jax
import jax.numpy as jnp
from jax import lax
from jax.experimental import pallas as pl
from jax.experimental.pallas import tpu as pltpu
from jax.sharding import PartitionSpec as P

ROTS = 16
MASKED = -1e30
PIECES = 4
PARTS = 2
LAST_PARTS = 8
NORM = 64
FLUSH = 4
MESH = pl.DeviceIdType.MESH


def exchange_kernel(
    sizes, ids_in, ctf_in, prec_in, prior_in, mask_in, images, templates,
    sums_ref, evid_ref,
    ids_ref, ctf_ref, prec_ref, prior_ref, mask_ref, grid_buf, tmpl, tnorm, base, act, all_w, all_p, own_stat, stat, fac,
    in_sem, tmpl_sem, own_sem, sent, c_recv, a_recv, p_recv, w_recv, s_recv, v_recv, up, side,
):
    Z, X, C, H, G, GL = sizes
    S = X * C
    g, z, x, c = [lax.axis_index(n) for n in ("groups", "img", "tpl", "sub")]
    refs, nb = tnorm.shape
    classes = refs // ROTS
    rows, pix = grid_buf.shape[2:]
    pb = pix // Z
    hr = rows // H
    s = x * C + c

    def chip(d):
        return lax.rem(x + d, X)

    def core(d):
        return lax.rem(c + d, C)

    def zoff(d):
        return lax.rem(z + d, Z)

    def dev(zz, xx, cc):
        return (g, zz, xx, cc)

    def hop(src, dst):
        return lax.rem(src - dst + Z - 1, Z)

    def scope(name):
        return jax.named_scope(name)

    peers = [(dx, dc) for dx in range(X) for dc in range(C) if dx or dc]
    inner = (z > 0) & (z < Z - 1)
    early = min(2, Z - 1)

    barrier = pltpu.get_barrier_semaphore()
    for dc in range(1, C):
        pl.semaphore_signal(barrier, inc=1, device_id=dev(z, x, core(dc)), device_id_type=MESH)

    @pl.loop(x + 1, X)
    def _(xx):
        for cc in range(C):
            pl.semaphore_signal(barrier, inc=1, device_id=dev(z, xx, cc), device_id_type=MESH)

    @pl.loop(z + 1, Z)
    def _(zz):
        pl.semaphore_signal(barrier, inc=1, device_id=dev(zz, x, c), device_id_type=MESH)

    started = []

    def local(src, dst, sem):
        cp = pltpu.make_async_copy(src, dst, sem)
        cp.start()
        return cp

    def copy(src, dst, send, recv, to):
        return pltpu.make_async_remote_copy(
            src_ref=src, dst_ref=dst, send_sem=send, recv_sem=recv, device_id=to, device_id_type=MESH
        )

    def remote(*args):
        cp = copy(*args)
        cp.start()
        started.append(cp)

    def arrive(dst, sem):
        pltpu.make_async_copy(dst, dst, sem).wait()

    small = [
        local(src, dst, in_sem.at[i])
        for i, (src, dst) in enumerate((
            (ids_in, ids_ref), (ctf_in, ctf_ref), (prec_in, prec_ref), (prior_in, prior_ref), (mask_in, mask_ref),
        ))
    ]
    tmpl_copy = local(templates, tmpl, tmpl_sem)
    own_copy = local(images, grid_buf.at[0, c], own_sem)

    with scope("barrier"):
        pl.semaphore_wait(barrier, C - 1 + x * C + z)

    @pl.loop(0, x)
    def _(xx):
        for cc in range(C):
            pl.semaphore_signal(side, inc=1, device_id=dev(z, xx, cc), device_id_type=MESH)

    @pl.loop(0, z)
    def _(zz):
        pl.semaphore_signal(up.at[jnp.where(zz == z - 1, 0, 1)], inc=1, device_id=dev(zz, x, c), device_id_type=MESH)

    def piece(i, cc, h):
        return grid_buf.at[i, cc, pl.ds(h * hr, hr), :]

    for dc in range(1, C):
        remote(images, grid_buf.at[0, c], sent, c_recv.at[C - dc - 1], dev(z, x, core(dc)))
    def p_block(zz, i, cc):
        return all_p.at[zz, i, cc]

    def p_copy(d):
        zz = zoff(d)
        cols = pl.ds(pl.multiple_of(zz * pb, pb), pb)
        return copy(images.at[:, cols], p_block(z, 0, c), sent, p_recv.at[hop(z, zz), 0], dev(zz, x, c))

    def outer(d):
        zz = zoff(d)
        return (zz == 0) | (zz == Z - 1)

    def crosses(zz):
        return (2 * z < Z) != (2 * zz < Z)

    def p_send_inner(n):
        for d in range(1, Z):
            over = crosses(zoff(d)) & jnp.logical_not(inner)
            first = (z == 0) & (zoff(d) == 1)
            slot = jnp.where(over, 1, 0)

            @pl.when(jnp.logical_not(outer(d) | first) & (slot == n))
            def _():
                p_copy(d).start()

    for d in range(1, Z):
        @pl.when(zoff(d) == 0)
        def _():
            p_copy(d).start()

    with scope("side"):
        @pl.when(x < X - 1)
        def _():
            pl.semaphore_wait(side, (X - 1 - x) * C)
    for h in range(H):
        for dx in range(1, X):
            remote(
                images.at[pl.ds(h * hr, hr), :], piece(X - dx, c, h), sent, a_recv.at[X - dx - 1, h],
                dev(z, chip(dx), c),
            )

    def wait_next():
        @pl.when(z < Z - 1)
        def _():
            pl.semaphore_wait(up.at[0], 1)

    def p_far():
        @pl.when(z < Z - 2)
        def _():
            pl.semaphore_wait(up.at[1], Z - 2 - z)

        for d in range(1, Z):
            @pl.when(zoff(d) == Z - 1)
            def _():
                p_copy(d).start()

    with scope("up"):
        if Z > 2:
            @pl.when(z == 0)
            def _():
                wait_next()
                p_copy(1).start()

            @pl.when(z > 0)
            def _():
                wait_next()
                p_far()

    with scope("small"):
        for cp in small:
            cp.wait()
    first = s * classes
    for i in range(classes):
        rws = pl.ds(i * ROTS, ROTS)
        base[rws, :] = jnp.full((ROTS, nb), prior_ref[first + i], jnp.float32)
        act[rws, :] = jnp.full((ROTS, nb), mask_ref[first + i], jnp.int32).astype(jnp.float32)

    factors, penalties = [], []
    for i in range(X):
        ids = ids_ref[chip(i)]
        ctf = jnp.zeros(ids.shape, jnp.float32)
        prec = ctf
        for q in range(ctf_ref.shape[0]):
            hit = ids == q
            ctf = jnp.where(hit, ctf_ref[q], ctf)
            prec = jnp.where(hit, prec_ref[q], prec)
        factors.append(prec * ctf)
        penalties.append(0.5 * prec * ctf * ctf)

    with scope("tmplw"):
        tmpl_copy.wait()

    with scope("tnorm"):
        @pl.loop(0, refs // NORM)
        def _(i):
            rws = pl.ds(pl.multiple_of(i * NORM, NORM), NORM)
            t = tmpl[rws, :].astype(jnp.float32)
            tnorm[rws, :] = jnp.broadcast_to(jnp.sum(t * t, axis=1, keepdims=True), (NORM, nb))

    def count(i):
        return GL if i == X - 1 else G

    def w_part(i, zz, q):
        n = refs // count(i)
        return all_w.at[i, zz, pl.ds(q * n, n), :]

    def w_sem(i, src, dst, q):
        return w_recv.at[hop(src, dst), i * G + q]

    def w_go(i, zz, q, right):
        to = lax.rem(z + (1 if right else -1) + Z, Z)
        return copy(w_part(i, zz, q), w_part(i, zz, q), sent, w_sem(i, zz, to, q), dev(to, x, c))

    def w_two(i, q):
        zz = lax.rem(jnp.where(z == 0, z + 2, z - 2) + Z, Z)
        return copy(w_part(i, z, q), w_part(i, z, q), sent, w_sem(i, z, zz, q), dev(zz, x, c))

    has_two = ((z == 0) | (z == Z - 1)) if Z > 2 else None

    def forwards(src, right):
        if right:
            return (z < Z - 1) & ((src > 0) | (z != 1))
        return (z > 0) & ((src < Z - 1) | (z != Z - 2))

    def sides(d, fn):
        @pl.when(z - d >= 0)
        def _():
            fn(z - d, True)

        @pl.when(z + d < Z)
        def _():
            fn(z + d, False)

    def w_forward(i, q):
        def fn(src, right):
            @pl.when(forwards(src, right))
            def _():
                with scope(f"wf{i}"):
                    arrive(w_part(i, src, q), w_sem(i, src, z, q))
                w_go(i, src, q, right).start()
        return fn

    def w_forwards(i, d, side, parts=None):
        def fn(src, right):
            if side is None or side == right:
                for q in parts or range(count(i)):
                    w_forward(i, q)(src, right)
        sides(d, fn)

    def w_wait(i, q):
        def fn(src, right):
            @pl.when(jnp.logical_not(forwards(src, right)))
            def _():
                with scope(f"ww{i}"):
                    arrive(w_part(i, src, q), w_sem(i, src, z, q))
        return fn

    def scores(i):
        pixels = grid_buf[i].reshape(nb, pix)
        raw = lax.dot_general(pixels, tmpl[...], (((1,), (1,)), ((), ())), preferred_element_type=jnp.float32).T
        live = act[...] > 0.0
        values = jnp.where(live, factors[i] * raw - penalties[i] * tnorm[...] + base[...], MASKED)
        peak = jnp.max(values, axis=0, keepdims=True)
        terms = jnp.where(live, jnp.exp(values - peak), 0.0)
        all_w[i, z] = terms.astype(jnp.bfloat16)
        total = jnp.sum(terms, axis=0, keepdims=True)
        row = lax.broadcasted_iota(jnp.int32, (8, nb), 0)
        own_stat[chip(i)] = jnp.where(row == 0, peak, total)

    def w_start(i):
        if Z > 2:
            @pl.when(has_two)
            def _():
                for q in range(count(i)):
                    w_two(i, q).start()

        for q in range(count(i)):
            @pl.when(z < Z - 1)
            def _():
                w_go(i, z, q, True).start()

            @pl.when(z > 0)
            def _():
                w_go(i, z, q, False).start()

    def p_forward(zz):
        out = []
        for dx in range(1, X):
            out.append(copy(p_block(zz, 0, c), p_block(zz, X - dx, c), sent, p_recv.at[hop(zz, z), X - dx], dev(z, chip(dx), c)))
        for dc in range(1, C):
            out.append(copy(p_block(zz, 0, c), p_block(zz, 0, c), sent, p_recv.at[hop(zz, z), X + C - 1 - dc], dev(z, x, core(dc))))
        return out

    def p_second(zz):
        out = []
        for dx in range(1, X):
            for dc in range(1, C):
                out.append(copy(p_block(zz, dx, c), p_block(zz, dx, c), sent, p_recv.at[hop(zz, z), X + C - 1 - dc], dev(z, x, core(dc))))
        return out

    def p_start(zz, right):
        with scope("pst"):
            arrive(p_block(zz, 0, c), p_recv.at[hop(zz, z), 0])
        for cp in p_forward(zz):
            cp.start()

    def p_slot(d, n):
        def fn(src, right):
            far = 3 if d == 1 else 2
            slot = jnp.where(inner & crosses(src), far, jnp.where(inner | (d == 1), 0, 1))

            @pl.when(slot == n)
            def _():
                p_start(src, right)
        sides(d, fn)

    def gather(dx, h):
        with scope(f"gath{h}"):
            arrive(piece(dx, c, h), a_recv.at[dx - 1, h])
        for dc in range(1, C):
            remote(piece(dx, c, h), piece(dx, c, h), sent, a_recv.at[dx - 1, H + C - 1 - dc], dev(z, x, core(dc)))

    own_copy.wait()
    with scope("own"):
        for dc in range(1, C):
            arrive(grid_buf.at[0, core(dc)], c_recv.at[dc - 1])
    with scope("sc0"):
        scores(0)

    @pl.when(z == 0)
    def _():
        if Z == 2:
            wait_next()
        p_far()

    w_start(0)
    if X == 1:
        p_send_inner(1)
    p_send_inner(0)

    for dx in range(1, X):
        for h in range(H // 2):
            gather(dx, h)
        for d in range(early, 1, -1):
            w_forwards(dx - 1, d, False)
        for h in range(H // 2, H - 1):
            gather(dx, h)
        for d in range(early, 1, -1):
            w_forwards(dx - 1, d, True, range(G - 1))
        w_forwards(dx - 1, 1, False, range(G // 2))
        gather(dx, H - 1)
        for d in range(early, 1, -1):
            w_forwards(dx - 1, d, True, range(G - 1, G))
        w_forwards(dx - 1, 1, False, range(G // 2, G))
        if dx == X - 1:
            p_send_inner(1)
            for d in range(1, early + 1):
                p_slot(d, 0)
        with scope(f"arrA{dx}"):
            for dc in range(1, C):
                arrive(grid_buf.at[dx, core(dc)], a_recv.at[dx - 1, H + dc - 1])
        with scope(f"sc{dx}"):
            scores(dx)
        w_start(dx)

    for dx, dc in peers:
        remote(own_stat, stat.at[s], sent, s_recv, dev(z, chip(dx), core(dc)))

    for i in range(X - 1):
        w_forwards(i, 1, True)
    for d in range(1, early + 1):
        p_slot(d, 1)

    @pl.loop(early + 1, Z)
    def _(d):
        sides(d, p_start)

    with scope("stat"):
        arrive(stat.at[pl.ds(0, S - 1)], s_recv)
    for i in range(X):
        xs = chip(i)
        own = own_stat[xs]
        parts = [(own[0:1], own[1:2])]
        for dx, dc in peers:
            got = stat[chip(dx) * C + core(dc), xs]
            parts.append((got[0:1], got[1:2]))
        peak = functools.reduce(jnp.maximum, [p for p, _ in parts])
        total = functools.reduce(jnp.add, [t * jnp.exp(p - peak) for p, t in parts])
        fac[z, i] = jnp.broadcast_to(factors[i] * jnp.exp(own[0:1] - peak) / total, (8, nb))
        if i == 0:
            evid = peak + jnp.log(total)
            mine = evid[:, 0:rows]
            for q in range(1, C):
                mine = jnp.where(c == q, evid[:, q * rows : (q + 1) * rows], mine)
            evid_ref[...] = mine
    for d in range(1, Z):
        remote(fac.at[z], fac.at[z], sent, v_recv.at[Z - d - 1], dev(zoff(d), x, c))

    def near(fn, over):
        def at(src, right):
            ok = crosses(src) if over else jnp.logical_not(crosses(src))

            @pl.when(ok)
            def _():
                fn(src, right)
        sides(1, at)

    def second_step(src, right):
        for dx in range(1, X):
            with scope("psec"):
                arrive(p_block(src, dx, c), p_recv.at[hop(src, z), dx])
        for cp in p_second(src):
            cp.start()

    def weights(zz, chunks, rws):
        return jnp.concatenate(
            [(all_w[i, zz, rws, :].astype(jnp.float32) * fac[zz, i, 0:1]).astype(jnp.bfloat16) for i in chunks], axis=1
        )

    def product(zz, chunks, rws):
        block = all_p[zz, chunks[0] : chunks[-1] + 1].reshape(len(chunks) * nb, pb)
        sums_ref[rws, :] += jnp.dot(weights(zz, chunks, rws), block, preferred_element_type=jnp.float32)

    def add_step(chunks):
        def fn(src, right):
            for i in chunks:
                for q in range(count(i)):
                    w_wait(i, q)(src, right)
            with scope("vw"):
                arrive(fac.at[src], v_recv.at[hop(src, z)])
            with scope("addw"):
                for dc in range(1, C):
                    arrive(all_p.at[src, :, core(dc)], p_recv.at[hop(src, z), X + dc - 1])
            with scope("addp"):
                product(src, chunks, pl.ds(0, refs))
        return fn

    def last_step(q):
        def fn(src, right):
            w_wait(X - 1, q)(src, right)
            with scope(f"last{q}"):
                product(src, range(X - 1, X), pl.ds(q * (refs // GL), refs // GL))
        return fn

    near(second_step, False)

    for d in range(early, 1, -1):
        p_slot(d, 2)
        w_forwards(X - 1, d, None)
    p_slot(1, 3)

    own_p = grid_buf[:, :, :, pl.ds(pl.multiple_of(z * pb, pb), pb)].reshape(X * nb, pb)
    with scope("prod0"):
        sums_ref[...] = jnp.dot(weights(z, range(X), pl.ds(0, refs)), own_p, preferred_element_type=jnp.float32)

    w_forwards(X - 1, 1, None)

    @pl.loop(early + 1, Z)
    def _(d):
        for i in range(X):
            w_forwards(i, d, None)

    def lasts(d):
        for q in range(GL):
            sides(d, last_step(q))

    @pl.loop(2, Z)
    def _(d):
        sides(d, second_step)

    near(add_step(range(X)), False)
    near(second_step, True)

    @pl.when(inner)
    def _():
        @pl.loop(2, Z)
        def _(d):
            sides(d, add_step(range(X)))

        near(add_step(range(X)), True)

    @pl.when(jnp.logical_not(inner))
    def _():
        @pl.loop(3, Z)
        def _(d):
            sides(d, add_step(range(X)))

        if Z > 2:
            sides(2, add_step(range(max(X - 1, 1))))
            if X > 1:
                lasts(2)
        else:
            near(add_step(range(X)), True)

    with scope("drain"):
        for cp in started:
            cp.wait_send()
        for d in range(1, Z):
            p_copy(d).wait_send()

        def end_step(src, right):
            for cp in p_forward(src) + p_second(src):
                cp.wait_send()
            for i in range(X):
                @pl.when(forwards(src, right))
                def _():
                    for q in range(count(i)):
                        w_go(i, src, q, right).wait_send()

        @pl.loop(1, Z)
        def _(d):
            sides(d, end_step)

        for i in range(X):
            for q in range(count(i)):
                if Z > 2:
                    @pl.when(has_two)
                    def _():
                        w_two(i, q).wait_send()

                @pl.when(z < Z - 1)
                def _():
                    w_go(i, z, q, True).wait_send()

                @pl.when(z > 0)
                def _():
                    w_go(i, z, q, False).wait_send()


def flush_kernel(sums, evid, sums_out, evid_out, sem):
    n = sem.shape[0] - 1
    step = sums.shape[0] // n
    copies = [pltpu.make_async_copy(evid, evid_out, sem.at[n])]
    for i in range(n):
        part = pl.ds(i * step, step)
        copies.append(pltpu.make_async_copy(sums.at[part, :], sums_out.at[part, :], sem.at[i]))
    for cp in copies:
        cp.start()
    for cp in copies:
        cp.wait()


def exchange(mesh, images, templates, group_ids, group_ctf, group_prec, log_prior, class_mask):
    Z, X, C = mesh.shape["img"], mesh.shape["tpl"], mesh.shape["sub"]
    S = X * C
    rows, pix = images.shape
    refs = templates.shape[0]
    nb = C * rows
    pb = pix // Z
    H, G, GL = PIECES, PARTS, LAST_PARTS
    vmem = pl.BlockSpec(memory_space=pltpu.VMEM)
    anyw = pl.BlockSpec(memory_space=pl.ANY)
    dma = pltpu.SemaphoreType.DMA
    f32, bf16 = jnp.float32, jnp.bfloat16
    class_sums, evid = pl.pallas_call(
        functools.partial(exchange_kernel, (Z, X, C, H, G, GL)),
        out_shape=(
            pltpu.VMEM((refs, pb), f32),
            pltpu.VMEM((1, rows), f32),
        ),
        in_specs=[anyw] * 7,
        out_specs=(vmem, vmem),
        scratch_shapes=[
            pltpu.VMEM((X, 1, nb), jnp.int32),
            pltpu.SMEM(group_ctf.shape, f32),
            pltpu.SMEM(group_prec.shape, f32),
            pltpu.SMEM(log_prior.shape, f32),
            pltpu.SMEM(class_mask.shape, jnp.int32),
            pltpu.VMEM((X, C, rows, pix), bf16),
            pltpu.VMEM((refs, pix), bf16),
            pltpu.VMEM((refs, nb), f32),
            pltpu.VMEM((refs, nb), f32),
            pltpu.VMEM((refs, nb), f32),
            pltpu.VMEM((X, Z, refs, nb), bf16),
            pltpu.VMEM((Z, X, C, rows, pb), bf16),
            pltpu.VMEM((X, 8, nb), f32),
            pltpu.VMEM((S, X, 8, nb), f32),
            pltpu.VMEM((Z, X, 8, nb), f32),
            dma((5,)), dma(()), dma(()), dma(()), dma((max(C - 1, 1),)), dma((max(X - 1, 1), H + C - 1)), dma((max(Z - 1, 1), X + C - 1)), dma((max(Z - 1, 1), (X - 1) * G + GL)), dma(()), dma((max(Z - 1, 1),)),
            pltpu.SemaphoreType.REGULAR((2,)), pltpu.SemaphoreType.REGULAR,
        ],
        compiler_params=pltpu.CompilerParams(
            collective_id=0, has_side_effects=True, vmem_limit_bytes=56 * 1024 * 1024
        ),
    )(group_ids.reshape(X, 1, nb), group_ctf, group_prec, log_prior, class_mask, images, templates)
    class_sums, evid = pl.pallas_call(
        flush_kernel,
        out_shape=(jax.ShapeDtypeStruct((refs, pb), f32), jax.ShapeDtypeStruct((1, rows), f32)),
        in_specs=[vmem, vmem],
        out_specs=(anyw, anyw),
        scratch_shapes=[dma((FLUSH + 1,))],
        compiler_params=pltpu.CompilerParams(vmem_limit_bytes=1024 * 1024),
    )(class_sums, evid)
    return class_sums, evid.reshape(rows)


def solution(mesh):
    placed = (
        P(("groups", "img", "tpl", "sub"), None),
        P(("groups", "tpl", "sub"), None),
        P(("groups", "img")),
        P("groups"),
        P("groups"),
        P("groups"),
        P("groups"),
    )
    return jax.shard_map(
        functools.partial(exchange, mesh),
        mesh=mesh,
        in_specs=placed,
        out_specs=(P(("groups", "tpl", "sub"), "img"), P(("groups", "img", "tpl", "sub"))),
        check_vma=False,
    )
```

```python
import functools
import jax
import jax.numpy as jnp
from jax import lax
from jax.experimental import pallas as pl
from jax.experimental.pallas import tpu as pltpu
from jax.sharding import PartitionSpec as P

ROTS = 16
MASKED = -1e30
PIECES = 4
PARTS = 2
LAST_PARTS = 8
NORM = 128
FLUSH = 1
MESH = pl.DeviceIdType.MESH


def exchange_kernel(
    sizes, ids_in, ctf_in, prec_in, prior_in, mask_in, images, templates,
    sums_ref, evid_ref,
    ids_ref, ctf_ref, prec_ref, prior_ref, mask_ref, grid_buf, tmpl, tnorm, base, act, all_w, all_p, own_stat, stat, fac,
    in_sem, tmpl_sem, own_sem, sent, c_recv, a_recv, p_recv, w_recv, s_recv, v_recv, up, side,
):
    Z, X, C, H, G, GL = sizes
    S = X * C
    g, z, x, c = [lax.axis_index(n) for n in ("groups", "img", "tpl", "sub")]
    refs, nb = tnorm.shape
    classes = refs // ROTS
    rows, pix = grid_buf.shape[2:]
    pb = pix // Z
    hr = rows // H
    s = x * C + c

    def chip(d):
        return lax.rem(x + d, X)

    def core(d):
        return lax.rem(c + d, C)

    def zoff(d):
        return lax.rem(z + d, Z)

    def dev(zz, xx, cc):
        return (g, zz, xx, cc)

    def hop(src, dst):
        return lax.rem(src - dst + Z - 1, Z)

    def scope(name):
        return jax.named_scope(name)

    peers = [(dx, dc) for dx in range(X) for dc in range(C) if dx or dc]
    inner = (z > 0) & (z < Z - 1)
    early = min(2, Z - 1)

    barrier = pltpu.get_barrier_semaphore()
    for dc in range(1, C):
        pl.semaphore_signal(barrier, inc=1, device_id=dev(z, x, core(dc)), device_id_type=MESH)

    @pl.loop(x + 1, X)
    def _(xx):
        for cc in range(C):
            pl.semaphore_signal(barrier, inc=1, device_id=dev(z, xx, cc), device_id_type=MESH)

    @pl.loop(z + 1, Z)
    def _(zz):
        pl.semaphore_signal(barrier, inc=1, device_id=dev(zz, x, c), device_id_type=MESH)

    started = []

    def local(src, dst, sem):
        cp = pltpu.make_async_copy(src, dst, sem)
        cp.start()
        return cp

    def copy(src, dst, send, recv, to):
        return pltpu.make_async_remote_copy(
            src_ref=src, dst_ref=dst, send_sem=send, recv_sem=recv, device_id=to, device_id_type=MESH
        )

    def remote(*args):
        cp = copy(*args)
        cp.start()
        started.append(cp)

    def arrive(dst, sem):
        pltpu.make_async_copy(dst, dst, sem).wait()

    small = [
        local(src, dst, in_sem.at[i])
        for i, (src, dst) in enumerate((
            (ids_in, ids_ref), (ctf_in, ctf_ref), (prec_in, prec_ref), (prior_in, prior_ref), (mask_in, mask_ref),
        ))
    ]
    tmpl_copy = local(templates, tmpl, tmpl_sem)
    own_copy = local(images, grid_buf.at[0, c], own_sem)

    with scope("barrier"):
        pl.semaphore_wait(barrier, C - 1 + x * C + z)

    @pl.loop(0, x)
    def _(xx):
        for cc in range(C):
            pl.semaphore_signal(side, inc=1, device_id=dev(z, xx, cc), device_id_type=MESH)

    @pl.loop(0, z)
    def _(zz):
        pl.semaphore_signal(up.at[jnp.where(zz == z - 1, 0, 1)], inc=1, device_id=dev(zz, x, c), device_id_type=MESH)

    def piece(i, cc, h):
        return grid_buf.at[i, cc, pl.ds(h * hr, hr), :]

    for dc in range(1, C):
        remote(images, grid_buf.at[0, c], sent, c_recv.at[C - dc - 1], dev(z, x, core(dc)))
    def p_block(zz, i, cc):
        return all_p.at[zz, i, cc]

    def p_copy(d):
        zz = zoff(d)
        cols = pl.ds(pl.multiple_of(zz * pb, pb), pb)
        return copy(images.at[:, cols], p_block(z, 0, c), sent, p_recv.at[hop(z, zz), 0], dev(zz, x, c))

    def outer(d):
        zz = zoff(d)
        return (zz == 0) | (zz == Z - 1)

    def crosses(zz):
        return (2 * z < Z) != (2 * zz < Z)

    def p_send_inner(n):
        for d in range(1, Z):
            over = crosses(zoff(d)) & jnp.logical_not(inner)
            first = (z == 0) & (zoff(d) == 1)
            slot = jnp.where(over, 1, 0)

            @pl.when(jnp.logical_not(outer(d) | first) & (slot == n))
            def _():
                p_copy(d).start()

    for d in range(1, Z):
        @pl.when(zoff(d) == 0)
        def _():
            p_copy(d).start()

    with scope("side"):
        @pl.when(x < X - 1)
        def _():
            pl.semaphore_wait(side, (X - 1 - x) * C)
    for h in range(H):
        for dx in range(1, X):
            remote(
                images.at[pl.ds(h * hr, hr), :], piece(X - dx, c, h), sent, a_recv.at[X - dx - 1, h],
                dev(z, chip(dx), c),
            )

    def wait_next():
        @pl.when(z < Z - 1)
        def _():
            pl.semaphore_wait(up.at[0], 1)

    def p_far():
        @pl.when(z < Z - 2)
        def _():
            pl.semaphore_wait(up.at[1], Z - 2 - z)

        for d in range(1, Z):
            @pl.when(zoff(d) == Z - 1)
            def _():
                p_copy(d).start()

    with scope("up"):
        if Z > 2:
            @pl.when(z == 0)
            def _():
                wait_next()
                p_copy(1).start()

            @pl.when(z > 0)
            def _():
                wait_next()
                p_far()

    with scope("small"):
        for cp in small:
            cp.wait()
    first = s * classes
    for i in range(classes):
        rws = pl.ds(i * ROTS, ROTS)
        base[rws, :] = jnp.full((ROTS, nb), prior_ref[first + i], jnp.float32)
        act[rws, :] = jnp.full((ROTS, nb), mask_ref[first + i], jnp.int32).astype(jnp.float32)

    factors, penalties = [], []
    for i in range(X):
        ids = ids_ref[chip(i)]
        ctf = jnp.zeros(ids.shape, jnp.float32)
        prec = ctf
        for q in range(ctf_ref.shape[0]):
            hit = ids == q
            ctf = jnp.where(hit, ctf_ref[q], ctf)
            prec = jnp.where(hit, prec_ref[q], prec)
        factors.append(prec * ctf)
        penalties.append(0.5 * prec * ctf * ctf)

    with scope("tmplw"):
        tmpl_copy.wait()

    with scope("tnorm"):
        @pl.loop(0, refs // NORM)
        def _(i):
            rws = pl.ds(pl.multiple_of(i * NORM, NORM), NORM)
            t = tmpl[rws, :].astype(jnp.float32)
            tnorm[rws, :] = jnp.broadcast_to(jnp.sum(t * t, axis=1, keepdims=True), (NORM, nb))

    def count(i):
        return GL if i == X - 1 else G

    def w_part(i, zz, q):
        n = refs // count(i)
        return all_w.at[i, zz, pl.ds(q * n, n), :]

    def w_sem(i, src, dst, q):
        return w_recv.at[hop(src, dst), i * G + q]

    def w_go(i, zz, q, right):
        to = lax.rem(z + (1 if right else -1) + Z, Z)
        return copy(w_part(i, zz, q), w_part(i, zz, q), sent, w_sem(i, zz, to, q), dev(to, x, c))

    def w_two(i, q):
        zz = lax.rem(jnp.where(z == 0, z + 2, z - 2) + Z, Z)
        return copy(w_part(i, z, q), w_part(i, z, q), sent, w_sem(i, z, zz, q), dev(zz, x, c))

    has_two = ((z == 0) | (z == Z - 1)) if Z > 2 else None

    def forwards(src, right):
        if right:
            return (z < Z - 1) & ((src > 0) | (z != 1))
        return (z > 0) & ((src < Z - 1) | (z != Z - 2))

    def sides(d, fn):
        @pl.when(z - d >= 0)
        def _():
            fn(z - d, True)

        @pl.when(z + d < Z)
        def _():
            fn(z + d, False)

    def w_forward(i, q):
        def fn(src, right):
            @pl.when(forwards(src, right))
            def _():
                with scope(f"wf{i}"):
                    arrive(w_part(i, src, q), w_sem(i, src, z, q))
                w_go(i, src, q, right).start()
        return fn

    def w_forwards(i, d, side, parts=None):
        def fn(src, right):
            if side is None or side == right:
                for q in parts or range(count(i)):
                    w_forward(i, q)(src, right)
        sides(d, fn)

    def w_wait(i, q):
        def fn(src, right):
            @pl.when(jnp.logical_not(forwards(src, right)))
            def _():
                with scope(f"ww{i}"):
                    arrive(w_part(i, src, q), w_sem(i, src, z, q))
        return fn

    def scores(i):
        pixels = grid_buf[i].reshape(nb, pix)
        raw = lax.dot_general(pixels, tmpl[...], (((1,), (1,)), ((), ())), preferred_element_type=jnp.float32).T
        live = act[...] > 0.0
        values = jnp.where(live, factors[i] * raw - penalties[i] * tnorm[...] + base[...], MASKED)
        peak = jnp.max(values, axis=0, keepdims=True)
        terms = jnp.where(live, jnp.exp(values - peak), 0.0)
        all_w[i, z] = terms.astype(jnp.bfloat16)
        total = jnp.sum(terms, axis=0, keepdims=True)
        row = lax.broadcasted_iota(jnp.int32, (8, nb), 0)
        own_stat[chip(i)] = jnp.where(row == 0, peak, total)

    def w_start(i):
        if Z > 2:
            @pl.when(has_two)
            def _():
                for q in range(count(i)):
                    w_two(i, q).start()

        for q in range(count(i)):
            @pl.when(z < Z - 1)
            def _():
                w_go(i, z, q, True).start()

            @pl.when(z > 0)
            def _():
                w_go(i, z, q, False).start()

    def p_forward(zz):
        out = []
        for dx in range(1, X):
            out.append(copy(p_block(zz, 0, c), p_block(zz, X - dx, c), sent, p_recv.at[hop(zz, z), X - dx], dev(z, chip(dx), c)))
        for dc in range(1, C):
            out.append(copy(p_block(zz, 0, c), p_block(zz, 0, c), sent, p_recv.at[hop(zz, z), X + C - 1 - dc], dev(z, x, core(dc))))
        return out

    def p_second(zz):
        out = []
        for dx in range(1, X):
            for dc in range(1, C):
                out.append(copy(p_block(zz, dx, c), p_block(zz, dx, c), sent, p_recv.at[hop(zz, z), X + C - 1 - dc], dev(z, x, core(dc))))
        return out

    def p_start(zz, right):
        with scope("pst"):
            arrive(p_block(zz, 0, c), p_recv.at[hop(zz, z), 0])
        for cp in p_forward(zz):
            cp.start()

    def p_slot(d, n):
        def fn(src, right):
            far = 3 if d == 1 else 2
            slot = jnp.where(inner & crosses(src), far, jnp.where(inner | (d == 1), 0, 1))

            @pl.when(slot == n)
            def _():
                p_start(src, right)
        sides(d, fn)

    def gather(dx, h):
        with scope(f"gath{h}"):
            arrive(piece(dx, c, h), a_recv.at[dx - 1, h])
        for dc in range(1, C):
            remote(piece(dx, c, h), piece(dx, c, h), sent, a_recv.at[dx - 1, H + C - 1 - dc], dev(z, x, core(dc)))

    own_copy.wait()
    with scope("own"):
        for dc in range(1, C):
            arrive(grid_buf.at[0, core(dc)], c_recv.at[dc - 1])
    with scope("sc0"):
        scores(0)

    @pl.when(z == 0)
    def _():
        if Z == 2:
            wait_next()
        p_far()

    w_start(0)
    if X == 1:
        p_send_inner(1)
    p_send_inner(0)

    for dx in range(1, X):
        for h in range(H // 2):
            gather(dx, h)
        for d in range(early, 1, -1):
            w_forwards(dx - 1, d, False)
        for h in range(H // 2, H - 1):
            gather(dx, h)
        for d in range(early, 1, -1):
            w_forwards(dx - 1, d, True, range(G - 1))
        w_forwards(dx - 1, 1, False, range(G // 2))
        gather(dx, H - 1)
        for d in range(early, 1, -1):
            w_forwards(dx - 1, d, True, range(G - 1, G))
        w_forwards(dx - 1, 1, False, range(G // 2, G))
        if dx == X - 1:
            p_send_inner(1)
            for d in range(1, early + 1):
                p_slot(d, 0)
        with scope(f"arrA{dx}"):
            for dc in range(1, C):
                arrive(grid_buf.at[dx, core(dc)], a_recv.at[dx - 1, H + dc - 1])
        with scope(f"sc{dx}"):
            scores(dx)
        w_start(dx)

    for dx, dc in peers:
        remote(own_stat, stat.at[s], sent, s_recv, dev(z, chip(dx), core(dc)))

    for i in range(X - 1):
        w_forwards(i, 1, True)
    for d in range(1, early + 1):
        p_slot(d, 1)

    @pl.loop(early + 1, Z)
    def _(d):
        sides(d, p_start)

    with scope("stat"):
        arrive(stat.at[pl.ds(0, S - 1)], s_recv)
    for i in range(X):
        xs = chip(i)
        own = own_stat[xs]
        parts = [(own[0:1], own[1:2])]
        for dx, dc in peers:
            got = stat[chip(dx) * C + core(dc), xs]
            parts.append((got[0:1], got[1:2]))
        peak = functools.reduce(jnp.maximum, [p for p, _ in parts])
        total = functools.reduce(jnp.add, [t * jnp.exp(p - peak) for p, t in parts])
        fac[z, i] = jnp.broadcast_to(factors[i] * jnp.exp(own[0:1] - peak) / total, (8, nb))
        if i == 0:
            evid = peak + jnp.log(total)
            mine = evid[:, 0:rows]
            for q in range(1, C):
                mine = jnp.where(c == q, evid[:, q * rows : (q + 1) * rows], mine)
            evid_ref[...] = mine
    for d in range(1, Z):
        remote(fac.at[z], fac.at[z], sent, v_recv.at[Z - d - 1], dev(zoff(d), x, c))

    def near(fn, over):
        def at(src, right):
            ok = crosses(src) if over else jnp.logical_not(crosses(src))

            @pl.when(ok)
            def _():
                fn(src, right)
        sides(1, at)

    def second_step(src, right):
        for dx in range(1, X):
            with scope("psec"):
                arrive(p_block(src, dx, c), p_recv.at[hop(src, z), dx])
        for cp in p_second(src):
            cp.start()

    def weights(zz, chunks, rws):
        return jnp.concatenate(
            [(all_w[i, zz, rws, :].astype(jnp.float32) * fac[zz, i, 0:1]).astype(jnp.bfloat16) for i in chunks], axis=1
        )

    def product(zz, chunks, rws):
        block = all_p[zz, chunks[0] : chunks[-1] + 1].reshape(len(chunks) * nb, pb)
        sums_ref[rws, :] += jnp.dot(weights(zz, chunks, rws), block, preferred_element_type=jnp.float32)

    def add_step(chunks):
        def fn(src, right):
            for i in chunks:
                for q in range(count(i)):
                    w_wait(i, q)(src, right)
            with scope("vw"):
                arrive(fac.at[src], v_recv.at[hop(src, z)])
            with scope("addw"):
                for dc in range(1, C):
                    arrive(all_p.at[src, :, core(dc)], p_recv.at[hop(src, z), X + dc - 1])
            with scope("addp"):
                product(src, chunks, pl.ds(0, refs))
        return fn

    def last_step(q):
        def fn(src, right):
            w_wait(X - 1, q)(src, right)
            with scope(f"last{q}"):
                product(src, range(X - 1, X), pl.ds(q * (refs // GL), refs // GL))
        return fn

    near(second_step, False)

    for d in range(early, 1, -1):
        p_slot(d, 2)
        w_forwards(X - 1, d, None)
    p_slot(1, 3)

    own_p = grid_buf[:, :, :, pl.ds(pl.multiple_of(z * pb, pb), pb)].reshape(X * nb, pb)
    with scope("prod0"):
        sums_ref[...] = jnp.dot(weights(z, range(X), pl.ds(0, refs)), own_p, preferred_element_type=jnp.float32)

    w_forwards(X - 1, 1, None)

    @pl.loop(early + 1, Z)
    def _(d):
        for i in range(X):
            w_forwards(i, d, None)

    def lasts(d):
        for q in range(GL):
            sides(d, last_step(q))

    @pl.loop(2, Z)
    def _(d):
        sides(d, second_step)

    near(add_step(range(X)), False)
    near(second_step, True)

    @pl.when(inner)
    def _():
        @pl.loop(2, Z)
        def _(d):
            sides(d, add_step(range(X)))

        near(add_step(range(X)), True)

    @pl.when(jnp.logical_not(inner))
    def _():
        @pl.loop(3, Z)
        def _(d):
            sides(d, add_step(range(X)))

        if Z > 2:
            sides(2, add_step(range(max(X - 1, 1))))
            if X > 1:
                lasts(2)
        else:
            near(add_step(range(X)), True)

    with scope("drain"):
        for cp in started:
            cp.wait_send()
        for d in range(1, Z):
            p_copy(d).wait_send()

        def end_step(src, right):
            for cp in p_forward(src) + p_second(src):
                cp.wait_send()
            for i in range(X):
                @pl.when(forwards(src, right))
                def _():
                    for q in range(count(i)):
                        w_go(i, src, q, right).wait_send()

        @pl.loop(1, Z)
        def _(d):
            sides(d, end_step)

        for i in range(X):
            for q in range(count(i)):
                if Z > 2:
                    @pl.when(has_two)
                    def _():
                        w_two(i, q).wait_send()

                @pl.when(z < Z - 1)
                def _():
                    w_go(i, z, q, True).wait_send()

                @pl.when(z > 0)
                def _():
                    w_go(i, z, q, False).wait_send()


def flush_kernel(sums, evid, sums_out, evid_out, sem):
    n = sem.shape[0] - 1
    step = sums.shape[0] // n
    copies = [pltpu.make_async_copy(evid, evid_out, sem.at[n])]
    for i in range(n):
        part = pl.ds(i * step, step)
        copies.append(pltpu.make_async_copy(sums.at[part, :], sums_out.at[part, :], sem.at[i]))
    for cp in copies:
        cp.start()
    for cp in copies:
        cp.wait()


def exchange(mesh, images, templates, group_ids, group_ctf, group_prec, log_prior, class_mask):
    Z, X, C = mesh.shape["img"], mesh.shape["tpl"], mesh.shape["sub"]
    S = X * C
    rows, pix = images.shape
    refs = templates.shape[0]
    nb = C * rows
    pb = pix // Z
    H, G, GL = PIECES, PARTS, LAST_PARTS
    vmem = pl.BlockSpec(memory_space=pltpu.VMEM)
    anyw = pl.BlockSpec(memory_space=pl.ANY)
    dma = pltpu.SemaphoreType.DMA
    f32, bf16 = jnp.float32, jnp.bfloat16
    class_sums, evid = pl.pallas_call(
        functools.partial(exchange_kernel, (Z, X, C, H, G, GL)),
        out_shape=(
            pltpu.VMEM((refs, pb), f32),
            pltpu.VMEM((1, rows), f32),
        ),
        in_specs=[anyw] * 7,
        out_specs=(vmem, vmem),
        scratch_shapes=[
            pltpu.VMEM((X, 1, nb), jnp.int32),
            pltpu.SMEM(group_ctf.shape, f32),
            pltpu.SMEM(group_prec.shape, f32),
            pltpu.SMEM(log_prior.shape, f32),
            pltpu.SMEM(class_mask.shape, jnp.int32),
            pltpu.VMEM((X, C, rows, pix), bf16),
            pltpu.VMEM((refs, pix), bf16),
            pltpu.VMEM((refs, nb), f32),
            pltpu.VMEM((refs, nb), f32),
            pltpu.VMEM((refs, nb), f32),
            pltpu.VMEM((X, Z, refs, nb), bf16),
            pltpu.VMEM((Z, X, C, rows, pb), bf16),
            pltpu.VMEM((X, 8, nb), f32),
            pltpu.VMEM((S, X, 8, nb), f32),
            pltpu.VMEM((Z, X, 8, nb), f32),
            dma((5,)), dma(()), dma(()), dma(()), dma((max(C - 1, 1),)), dma((max(X - 1, 1), H + C - 1)), dma((max(Z - 1, 1), X + C - 1)), dma((max(Z - 1, 1), (X - 1) * G + GL)), dma(()), dma((max(Z - 1, 1),)),
            pltpu.SemaphoreType.REGULAR((2,)), pltpu.SemaphoreType.REGULAR,
        ],
        compiler_params=pltpu.CompilerParams(
            collective_id=0, has_side_effects=True, vmem_limit_bytes=56 * 1024 * 1024
        ),
    )(group_ids.reshape(X, 1, nb), group_ctf, group_prec, log_prior, class_mask, images, templates)
    class_sums, evid = pl.pallas_call(
        flush_kernel,
        out_shape=(jax.ShapeDtypeStruct((refs, pb), f32), jax.ShapeDtypeStruct((1, rows), f32)),
        in_specs=[vmem, vmem],
        out_specs=(anyw, anyw),
        scratch_shapes=[dma((FLUSH + 1,))],
        compiler_params=pltpu.CompilerParams(vmem_limit_bytes=1024 * 1024),
    )(class_sums, evid)
    return class_sums, evid.reshape(rows)


def solution(mesh):
    placed = (
        P(("groups", "img", "tpl", "sub"), None),
        P(("groups", "tpl", "sub"), None),
        P(("groups", "img")),
        P("groups"),
        P("groups"),
        P("groups"),
        P("groups"),
    )
    return jax.shard_map(
        functools.partial(exchange, mesh),
        mesh=mesh,
        in_specs=placed,
        out_specs=(P(("groups", "tpl", "sub"), "img"), P(("groups", "img", "tpl", "sub"))),
        check_vma=False,
    )
```
